256 devices in a mesh: layer: 2 (over core), ex: 128 (over z, y, x).
Axes of the slice: x: 4, y: 4, z: 8, core: 2. Of those that a mesh axis runs over, the one named last changes fastest.
Arguments:
- grads: bfloat16 [2, 32768, 512], P('layer', 'ex'), may hold values from -6 to 6
- labeled: int32 [32768], P('ex'), may hold values 0 or 1
- damping: float32 [2], P('layer'), may hold values from 0.05 to 0.5
Outputs:
- solved: float32 [2, 32768, 512], P('layer', 'ex')
- score: float32 [32768], P('ex')
The draws below stay inside these ranges and needn't reach their ends.
All inputs are finite; a program needn't handle non-finite values. No bound on the sum of `labeled` on one device may be relied on, other than what follows from the above.
Results may differ from the reference program's by a relative error of at most 0.0003.
Values may be sent and summed in bfloat16 or wider, within the bound.
No kernel may reach another device: no remote copies, remote signals or barrier semaphores. Data moves between devices by JAX's collectives and lax.ppermute only.
A program may use at most 64 MiB of HBM per device.

```python
import math
import jax
import jax.numpy as jnp
from jax import lax

K = 512
LAYERS = 2
CAND = 32768


def draw_grads(key, part):
    first = jax.random.fold_in(key, 0)
    fresh_noise = jax.random.normal(first, (LAYERS, CAND, K), jnp.float32)

    def mixing(previous, incoming):
        current = 0.6 * previous + 0.8 * incoming
        return (current, current)
    finished, mixed = lax.scan(mixing, jnp.zeros((CAND, K), jnp.float32), fresh_noise)
    return jnp.clip(mixed, -6.0, 6.0).astype(jnp.bfloat16)


def touch_ends(values, own_key, smallest, top_value):
    extent = values.shape
    spot = [jax.random.randint(jax.random.fold_in(own_key, axis), (), 0, extent[axis]) for axis in range(len(extent))]
    values = values.at[tuple(spot)].set(smallest)
    longest = extent.index(max(extent))
    spot[longest] = (spot[longest] + 1) % extent[longest]
    return values.at[tuple(spot)].set(top_value)


def block_levels(rng, dims, cuts, low, top_value):
    level, own = 1.0, jax.random.fold_in(rng, 6)
    for axis_at, parts in cuts:
        steps = jnp.exp(jax.random.uniform(jax.random.fold_in(own, axis_at), (parts,), jnp.float32, low / len(cuts), top_value / len(cuts)))
        level = level * jnp.repeat(steps, dims[axis_at] // parts).reshape([-1 if axis == axis_at else 1 for axis in range(len(dims))])
    return level


def setup_inputs(seed: int = 0) -> dict:
    arg_keys = jax.random.split(jax.random.key(seed), 4)
    grads = draw_grads(jax.random.fold_in(arg_keys[3], 71), 0)
    labeled = touch_ends((jax.random.randint(arg_keys[1], (CAND,), 0, 2) < 1).astype(jnp.int32), jax.random.fold_in(arg_keys[1], 1), 0, 1)
    damping = jnp.clip(jnp.exp(math.log(0.5) - 2.3025851 * jax.random.uniform(arg_keys[2], (LAYERS,), jnp.float32) ** block_levels(arg_keys[2], (LAYERS,), ((0, 2),), -0.2, 0.2)), 0.05, 0.5)
    return dict(grads=grads, labeled=labeled, damping=damping)


def lower_solve(factor, right_hand):
    return jax.scipy.linalg.solve_triangular(factor, right_hand, lower=True)

def apply_inverse(factor, row_block):
    inner = jax.scipy.linalg.solve_triangular(factor, row_block.T, lower=True)
    return jax.scipy.linalg.solve_triangular(factor, inner, lower=True, trans=1).T

def reference(grads, labeled, damping):
    layer_count, cand_count, sketch_width = grads.shape
    keep_mask = (labeled > 0)[None, :, None]
    masked = jnp.where(keep_mask, grads, jnp.zeros_like(grads))
    identity = jnp.eye(sketch_width, dtype=jnp.float32)
    factor = identity
    trail = jnp.zeros((cand_count, sketch_width), jnp.float32)
    factors = []
    lefts = []
    couplings = []
    for layer in range(layer_count):
        diagonal = jnp.dot(masked[layer].T.astype(jnp.float32), grads[layer].astype(jnp.float32), preferred_element_type=jnp.float32) / cand_count + damping[layer] * identity
        if layer > 0:
            coupling = jnp.dot(masked[layer - 1].T.astype(jnp.float32), grads[layer].astype(jnp.float32), preferred_element_type=jnp.float32) / cand_count
        else:
            coupling = jnp.zeros((sketch_width, sketch_width), jnp.float32)
        cross = lower_solve(factor, coupling)
        schur = diagonal - jnp.dot(cross.T, cross, precision=lax.Precision.HIGHEST)
        left_side = grads[layer].astype(jnp.float32) - jnp.dot(trail, coupling, precision=lax.Precision.HIGHEST)
        factor = jnp.linalg.cholesky(schur)
        trail = apply_inverse(factor, left_side)
        factors.append(factor)
        lefts.append(left_side)
        couplings.append(coupling)
    flow = jnp.zeros((cand_count, sketch_width), jnp.float32)
    solved = [None] * layer_count
    gain = jnp.zeros((cand_count,), jnp.float32)
    penalty = jnp.zeros((cand_count,), jnp.float32)
    for layer in reversed(range(layer_count)):
        vector = apply_inverse(factors[layer], lefts[layer] - flow)
        flow = jnp.dot(vector, couplings[layer].T, precision=lax.Precision.HIGHEST)
        solved[layer] = vector
        gain = gain + jnp.sum(grads[layer].astype(jnp.float32) * vector, axis=1)
        penalty = penalty + damping[layer] * jnp.sum(vector * vector, axis=1)
    score = (gain - penalty) / (1.0 + gain)
    return (jnp.stack(solved), score)
```

```python
import functools

import jax
import jax.numpy as jnp
from jax import lax
from jax.experimental import pallas as pl
from jax.experimental.pallas import tpu as pltpu
from jax.sharding import Mesh
from jax.sharding import PartitionSpec as P

EX = ("ex_0", "ex_1", "ex_2")
F32, BF16 = jnp.float32, jnp.bfloat16
LANES = 128
RESIDUAL = 0.008
STEPS = 60


def dot(a, b, dims=((1,), (0,)), precision=None):
    return lax.dot_general(a, b, (dims, ((), ())), preferred_element_type=F32, precision=precision)


def split(a):
    high = a.astype(BF16)
    return high, (a - high.astype(F32)).astype(BF16)


def dot_split(a, b, dims=((1,), (0,))):
    total = dot(a[0], b[0], dims)
    if len(b) > 1:
        total = total + dot(a[0], b[1], dims)
    if len(a) > 1:
        total = total + dot(a[1], b[0], dims)
    return total


def gram_kernel(width, core_ref, labeled_ref, own_ref, other_ref, out_ref):
    blocks = width // LANES
    core = core_ref[0]
    keep = (labeled_ref[...] > 0).astype(F32)
    own, other = own_ref[...], other_ref[...]
    own_t = (own.astype(F32).T * keep).astype(BF16)
    first_t = jnp.where(core == 0, own_t, (other.astype(F32).T * keep).astype(BF16))
    last = jnp.where(core == 0, other, own)
    both = jnp.concatenate([own, other], axis=1)
    slab = blocks * LANES + LANES // 2
    for i in range(blocks):
        rows = own_t[i * LANES : (i + 1) * LANES]
        product = dot(rows, both[:, i * LANES : (i + blocks) * LANES])
        for b in range(blocks):
            start = i * slab + b * LANES
            out_ref[start : start + LANES] = product[:, b * LANES : (b + 1) * LANES]
        middle = dot(first_t[i * LANES : (i + 1) * LANES], last[:, i * LANES : (i + 1) * LANES])
        start = i * slab + blocks * LANES
        half = LANES // 2
        out_ref[start : start + half] = jnp.where(core == 0, middle[:half], middle[half:])


def sum_kernel(parts, copies, in_ref, out_ref):
    rows = in_ref.shape[0] // parts
    total = in_ref[:rows]
    for part in range(1, parts):
        total = total + in_ref[part * rows : (part + 1) * rows]
    for copy in range(copies):
        out_ref[copy * rows : (copy + 1) * rows] = total


def eye(width):
    rows = lax.broadcasted_iota(jnp.int32, (width, width), 0)
    return rows == lax.broadcasted_iota(jnp.int32, (width, width), 1)


def invert(s_ref, a_ref, x_ref, r_ref):
    width = s_ref.shape[0]
    unit = eye(width)
    one = unit.astype(F32)
    diagonal = jnp.where(unit, s_ref[...], 0.0)
    scale_row = lax.rsqrt(jnp.sum(diagonal, axis=0, keepdims=True))
    scale_col = lax.rsqrt(jnp.sum(diagonal, axis=1, keepdims=True))
    a_ref[...] = s_ref[...] * scale_col * scale_row

    e = one - a_ref[...]
    e1 = e.astype(BF16)
    e2 = dot(e1, e1).astype(BF16)
    x_ref[...] = one + e
    x_ref[...] += dot(x_ref[...].astype(BF16), e2)
    e4 = dot(e2, e2)
    x_ref[...] += dot(x_ref[...].astype(BF16), e4.astype(BF16))
    contracts = jnp.sum(e4 * e4) < 0.1

    @pl.when(jnp.logical_not(contracts))
    def _():
        largest = jnp.max(jnp.sum(jnp.abs(a_ref[...]), axis=1, keepdims=True))
        x_ref[...] = jnp.where(unit, 1.0 / largest, 0.0)

    r_ref[...] = one - dot_split(split(a_ref[...]), split(x_ref[...]))

    def far(state):
        step, norm = state
        return jnp.logical_and(step < STEPS, norm > RESIDUAL**2)

    def newton(state):
        tile = width // 4

        def advance(t, _):
            at = pl.ds(pl.multiple_of(t * tile, tile), tile)
            x_ref[at, :] += dot(x_ref[at, :], r_ref[...], precision=lax.Precision.HIGHEST)
            return 0

        def residual(t, _):
            at = pl.ds(pl.multiple_of(t * tile, tile), tile)
            r_ref[at, :] = -dot(a_ref[at, :], x_ref[...], precision=lax.Precision.HIGHEST)
            return 0

        lax.fori_loop(0, 4, advance, 0)
        lax.fori_loop(0, 4, residual, 0)
        r_ref[...] += eye(width).astype(F32)
        return state[0] + 1, jnp.sum(r_ref[...] * r_ref[...])

    lax.while_loop(far, newton, (jnp.int32(0), jnp.sum(r_ref[...] * r_ref[...])))
    x_ref[...] += dot(x_ref[...].astype(BF16), r_ref[...].astype(BF16))
    x_ref[...] = x_ref[...] * scale_col * scale_row


def solve_kernel(
    count, core_ref, damp_ref, mine_ref, theirs_ref, own_ref, other_ref,
    solved_ref, score_ref, s_ref, c_ref, ct_ref, d1_ref, a_ref, x_ref, r_ref, y_ref, p0_ref,
):
    core = core_ref[0]
    width = own_ref.shape[1]
    blocks = width // LANES
    half = LANES // 2
    slab = blocks * LANES + half
    near = core == 0
    damp0 = jnp.where(near, damp_ref[0], damp_ref[1])
    damp1 = jnp.where(near, damp_ref[1], damp_ref[0])

    def part(layer, i, start, rows):
        at = i * slab + start
        mine, theirs = mine_ref[at : at + rows], theirs_ref[at : at + rows]
        first, second = (mine, theirs) if layer == 0 else (theirs, mine)
        return jnp.where(near, first, second) * (1.0 / count)

    def put(ref, i, j, block):
        ref[i * LANES : (i + 1) * LANES, j * LANES : (j + 1) * LANES] = block

    unit = eye(LANES)
    for layer, ref, damp in ((0, s_ref, damp0), (1, d1_ref, damp1)):
        for i in range(blocks):
            for b in range(blocks):
                block = part(layer, i, b * LANES, LANES)
                j = i + b
                if b == 0:
                    put(ref, i, i, block + jnp.where(unit, damp, 0.0))
                elif j < blocks:
                    put(ref, i, j, block)
                    put(ref, j, i, block.T)
                elif layer == 0:
                    put(c_ref, i, j - blocks, block)
                    put(ct_ref, j - blocks, i, block.T)
                else:
                    put(ct_ref, i, j - blocks, block)
                    put(c_ref, j - blocks, i, block.T)
    for i in range(blocks):
        block = jnp.concatenate([part(0, i, blocks * LANES, half), part(1, i, blocks * LANES, half)], 0)
        put(c_ref, i, i, block)
        put(ct_ref, i, i, block.T)

    def section(layer, _):
        invert(s_ref, a_ref, x_ref, r_ref)

        @pl.when(layer == 0)
        def _():
            p0_ref[...] = x_ref[...]
            y_ref[...] = dot_split(split(x_ref[...]), split(c_ref[...]))
            s_ref[...] = d1_ref[...] - dot_split(split(ct_ref[...]), split(y_ref[...]))

        return 0

    lax.fori_loop(0, 2, section, 0)
    own, other = own_ref[...], other_ref[...]
    g0 = jnp.where(near, own, other)
    g1 = jnp.where(near, other, own)
    y = split(y_ref[...])
    left = g1.astype(F32) - dot_split((g0,), y)
    z1 = dot_split(split(left), split(x_ref[...]))
    z0 = dot_split((g0,), split(p0_ref[...])) - dot_split(split(z1), y, ((1,), (1,)))
    solved_ref[...] = jnp.where(near, z0, z1)
    gain = g0.astype(F32) * z0 + g1.astype(F32) * z1
    penalty = damp0 * (z0 * z0) + damp1 * (z1 * z1)

    def candidate_sum(terms):
        folded = terms[:, :LANES]
        for b in range(1, blocks):
            folded = folded + terms[:, b * LANES : (b + 1) * LANES]
        return jnp.sum(folded.T, axis=0, keepdims=True)

    gain, penalty = candidate_sum(gain), candidate_sum(penalty)
    score_ref[...] = (gain - penalty) / (1.0 + gain)


SMEM = pl.BlockSpec(memory_space=pltpu.SMEM)
VMEM = pl.BlockSpec(memory_space=pltpu.VMEM)


def exchanged(array, axis):
    devices = lax.axis_size(axis)
    parts = lax.all_to_all(array.reshape(devices, 1, -1), axis, 0, 0, tiled=True)
    return parts.reshape(array.shape)


def on_device(grads, labeled, damping):
    _, row_count, width = grads.shape
    count = row_count * lax.axis_size(EX)
    core = lax.axis_index("layer").astype(jnp.int32).reshape(1)
    swap = [(0, 1), (1, 0)]
    own = grads[0]
    other = lax.ppermute(own, "layer", swap)
    damp = jnp.concatenate([damping, lax.ppermute(damping, "layer", swap)])
    blocks = width // LANES
    slab = blocks * LANES + LANES // 2
    far, near = lax.axis_size(("ex_0", "ex_1")), lax.axis_size("ex_2")

    products = pl.pallas_call(
        functools.partial(gram_kernel, width),
        out_shape=jax.ShapeDtypeStruct((blocks * slab, LANES), F32),
        in_specs=[SMEM, VMEM, VMEM, VMEM],
        out_specs=VMEM,
    )(core, labeled.reshape(1, row_count), own, other)
    arrived = exchanged(products, "ex_2")
    slab_part = pl.pallas_call(
        functools.partial(sum_kernel, near, 1),
        out_shape=jax.ShapeDtypeStruct((slab, LANES), F32),
        in_specs=[VMEM],
        out_specs=VMEM,
    )(arrived)
    arrived = exchanged(slab_part, ("ex_0", "ex_1"))
    piece = pl.pallas_call(
        functools.partial(sum_kernel, far, far),
        out_shape=jax.ShapeDtypeStruct((slab, LANES), F32),
        in_specs=[VMEM],
        out_specs=VMEM,
    )(arrived)
    whole = exchanged(piece, ("ex_0", "ex_1"))
    copies = jnp.broadcast_to(whole[None], (near, slab, LANES)).reshape(near * slab, LANES)
    mine = exchanged(copies, "ex_2")
    theirs = lax.ppermute(mine, "layer", swap)

    square = pltpu.VMEM((width, width), F32)
    solved, score = pl.pallas_call(
        functools.partial(solve_kernel, count),
        out_shape=(
            jax.ShapeDtypeStruct((row_count, width), F32),
            jax.ShapeDtypeStruct((1, row_count), F32),
        ),
        in_specs=[SMEM, SMEM, VMEM, VMEM, VMEM, VMEM],
        out_specs=(VMEM, VMEM),
        scratch_shapes=[square] * 9,
    )(core, damp, mine, theirs, own, other)
    return solved[None], score.reshape(row_count)


def solution(mesh):
    torus = Mesh(
        mesh.devices.reshape(mesh.shape["layer"], 8, 4, 4), ("layer", "ex_0", "ex_1", "ex_2")
    )
    in_specs = (P("layer", EX, None), P(EX), P("layer"))
    out_specs = (P("layer", EX, None), P(EX))
    return jax.shard_map(
        on_device, mesh=torus, in_specs=in_specs, out_specs=out_specs, check_vma=False
    )
```

```python
import functools

import jax
import jax.numpy as jnp
from jax import lax
from jax.experimental import pallas as pl
from jax.experimental.pallas import tpu as pltpu
from jax.sharding import Mesh
from jax.sharding import PartitionSpec as P

EX = ("ex_0", "ex_1", "ex_2")
F32, BF16 = jnp.float32, jnp.bfloat16
LANES = 128
RESIDUAL = 0.008
STEPS = 60


def dot(a, b, dims=((1,), (0,)), precision=None):
    return lax.dot_general(a, b, (dims, ((), ())), preferred_element_type=F32, precision=precision)


def split(a):
    high = a.astype(BF16)
    return high, (a - high.astype(F32)).astype(BF16)


def dot_split(a, b, dims=((1,), (0,))):
    total = dot(a[0], b[0], dims)
    if len(b) > 1:
        total = total + dot(a[0], b[1], dims)
    if len(a) > 1:
        total = total + dot(a[1], b[0], dims)
    return total


def gram_kernel(width, core_ref, labeled_ref, own_ref, other_ref, out_ref):
    blocks = width // LANES
    core = core_ref[0]
    keep = (labeled_ref[...] > 0).astype(F32)
    own, other = own_ref[...], other_ref[...]
    own_t = (own.astype(F32).T * keep).astype(BF16)
    first_t = jnp.where(core == 0, own_t, (other.astype(F32).T * keep).astype(BF16))
    last = jnp.where(core == 0, other, own)
    both = jnp.concatenate([own, other], axis=1)
    slab = blocks * LANES + LANES // 2
    for i in range(blocks):
        rows = own_t[i * LANES : (i + 1) * LANES]
        product = dot(rows, both[:, i * LANES : (i + blocks) * LANES])
        for b in range(blocks):
            start = i * slab + b * LANES
            out_ref[start : start + LANES] = product[:, b * LANES : (b + 1) * LANES]
        middle = dot(first_t[i * LANES : (i + 1) * LANES], last[:, i * LANES : (i + 1) * LANES])
        start = i * slab + blocks * LANES
        half = LANES // 2
        out_ref[start : start + half] = jnp.where(core == 0, middle[:half], middle[half:])


def sum_kernel(parts, copies, in_ref, out_ref):
    rows = in_ref.shape[0] // parts
    total = in_ref[:rows]
    for part in range(1, parts):
        total = total + in_ref[part * rows : (part + 1) * rows]
    for copy in range(copies):
        out_ref[copy * rows : (copy + 1) * rows] = total


def eye(width):
    rows = lax.broadcasted_iota(jnp.int32, (width, width), 0)
    return rows == lax.broadcasted_iota(jnp.int32, (width, width), 1)


def invert(s_ref, a_ref, x_ref, r_ref):
    width = s_ref.shape[0]
    unit = eye(width)
    one = unit.astype(F32)
    diagonal = jnp.where(unit, s_ref[...], 0.0)
    scale_row = lax.rsqrt(jnp.sum(diagonal, axis=0, keepdims=True))
    scale_col = lax.rsqrt(jnp.sum(diagonal, axis=1, keepdims=True))
    a_ref[...] = s_ref[...] * scale_col * scale_row

    e = one - a_ref[...]
    e1 = e.astype(BF16)
    e2 = dot(e1, e1).astype(BF16)
    x_ref[...] = one + e
    x_ref[...] += dot(x_ref[...].astype(BF16), e2)
    e4 = dot(e2, e2)
    x_ref[...] += dot(x_ref[...].astype(BF16), e4.astype(BF16))
    contracts = jnp.sum(e4 * e4) < 0.1

    @pl.when(jnp.logical_not(contracts))
    def _():
        largest = jnp.max(jnp.sum(jnp.abs(a_ref[...]), axis=1, keepdims=True))
        x_ref[...] = jnp.where(unit, 1.0 / largest, 0.0)

    r_ref[...] = one - dot_split(split(a_ref[...]), split(x_ref[...]))

    def far(state):
        step, norm = state
        return jnp.logical_and(step < STEPS, norm > RESIDUAL**2)

    def newton(state):
        tile = width // 4

        def advance(t, _):
            at = pl.ds(pl.multiple_of(t * tile, tile), tile)
            x_ref[at, :] += dot(x_ref[at, :], r_ref[...], precision=lax.Precision.HIGHEST)
            return 0

        def residual(t, _):
            at = pl.ds(pl.multiple_of(t * tile, tile), tile)
            r_ref[at, :] = -dot(a_ref[at, :], x_ref[...], precision=lax.Precision.HIGHEST)
            return 0

        lax.fori_loop(0, 4, advance, 0)
        lax.fori_loop(0, 4, residual, 0)
        r_ref[...] += eye(width).astype(F32)
        return state[0] + 1, jnp.sum(r_ref[...] * r_ref[...])

    lax.while_loop(far, newton, (jnp.int32(0), jnp.sum(r_ref[...] * r_ref[...])))
    x_ref[...] += dot(x_ref[...].astype(BF16), r_ref[...].astype(BF16))
    x_ref[...] = x_ref[...] * scale_col * scale_row


def solve_kernel(
    count, core_ref, damp_ref, damp_other_ref, mine_ref, theirs_ref, own_ref, other_ref,
    solved_ref, score_ref, s_ref, c_ref, ct_ref, d1_ref, a_ref, x_ref, r_ref, y_ref, p0_ref,
):
    core = core_ref[0]
    width = own_ref.shape[1]
    blocks = width // LANES
    half = LANES // 2
    slab = blocks * LANES + half
    near = core == 0
    damp0 = jnp.where(near, damp_ref[0], damp_other_ref[0])
    damp1 = jnp.where(near, damp_other_ref[0], damp_ref[0])

    def part(layer, i, start, rows):
        at = i * slab + start
        mine, theirs = mine_ref[at : at + rows], theirs_ref[at : at + rows]
        first, second = (mine, theirs) if layer == 0 else (theirs, mine)
        return jnp.where(near, first, second) * (1.0 / count)

    def put(ref, i, j, block):
        ref[i * LANES : (i + 1) * LANES, j * LANES : (j + 1) * LANES] = block

    unit = eye(LANES)
    for layer, ref, damp in ((0, s_ref, damp0), (1, d1_ref, damp1)):
        for i in range(blocks):
            for b in range(blocks):
                block = part(layer, i, b * LANES, LANES)
                j = i + b
                if b == 0:
                    put(ref, i, i, block + jnp.where(unit, damp, 0.0))
                elif j < blocks:
                    put(ref, i, j, block)
                    put(ref, j, i, block.T)
                elif layer == 0:
                    put(c_ref, i, j - blocks, block)
                    put(ct_ref, j - blocks, i, block.T)
                else:
                    put(ct_ref, i, j - blocks, block)
                    put(c_ref, j - blocks, i, block.T)
    for i in range(blocks):
        block = jnp.concatenate([part(0, i, blocks * LANES, half), part(1, i, blocks * LANES, half)], 0)
        put(c_ref, i, i, block)
        put(ct_ref, i, i, block.T)

    def section(layer, _):
        invert(s_ref, a_ref, x_ref, r_ref)

        @pl.when(layer == 0)
        def _():
            p0_ref[...] = x_ref[...]
            y_ref[...] = dot_split(split(x_ref[...]), split(c_ref[...]))
            s_ref[...] = d1_ref[...] - dot_split(split(ct_ref[...]), split(y_ref[...]))

        return 0

    lax.fori_loop(0, 2, section, 0)
    own, other = own_ref[...], other_ref[...]
    g0 = jnp.where(near, own, other)
    g1 = jnp.where(near, other, own)
    y = split(y_ref[...])
    left = g1.astype(F32) - dot_split((g0,), y)
    z1 = dot_split(split(left), split(x_ref[...]))
    z0 = dot_split((g0,), split(p0_ref[...])) - dot_split(split(z1), y, ((1,), (1,)))
    solved_ref[...] = jnp.where(near, z0, z1)
    gain = g0.astype(F32) * z0 + g1.astype(F32) * z1
    penalty = damp0 * (z0 * z0) + damp1 * (z1 * z1)

    def candidate_sum(terms):
        folded = terms[:, :LANES]
        for b in range(1, blocks):
            folded = folded + terms[:, b * LANES : (b + 1) * LANES]
        return jnp.sum(folded.T, axis=0, keepdims=True)

    gain, penalty = candidate_sum(gain), candidate_sum(penalty)
    score_ref[...] = (gain - penalty) / (1.0 + gain)


SMEM = pl.BlockSpec(memory_space=pltpu.SMEM)
VMEM = pl.BlockSpec(memory_space=pltpu.VMEM)


def exchanged(array, axis):
    devices = lax.axis_size(axis)
    parts = lax.all_to_all(array.reshape(devices, 1, -1), axis, 0, 0, tiled=True)
    return parts.reshape(array.shape)


def on_device(grads, labeled, damping):
    _, row_count, width = grads.shape
    count = row_count * lax.axis_size(EX)
    core = lax.axis_index("layer").astype(jnp.int32).reshape(1)
    swap = [(0, 1), (1, 0)]
    own = grads[0]
    other = lax.ppermute(own, "layer", swap)
    damp = lax.ppermute(damping, "layer", swap)
    blocks = width // LANES
    slab = blocks * LANES + LANES // 2
    far, near = lax.axis_size("ex_0"), lax.axis_size(("ex_1", "ex_2"))

    piece_rows = blocks * slab // near

    products = pl.pallas_call(
        functools.partial(gram_kernel, width),
        out_shape=jax.ShapeDtypeStruct((blocks * slab, LANES), F32),
        in_specs=[SMEM, VMEM, VMEM, VMEM],
        out_specs=VMEM,
    )(core, labeled.reshape(1, row_count), own, other)
    arrived = exchanged(products, ("ex_1", "ex_2"))
    slab_part = pl.pallas_call(
        functools.partial(sum_kernel, near, 1),
        out_shape=jax.ShapeDtypeStruct((piece_rows, LANES), F32),
        in_specs=[VMEM],
        out_specs=VMEM,
    )(arrived)
    arrived = exchanged(slab_part, "ex_0")
    piece = pl.pallas_call(
        functools.partial(sum_kernel, far, far),
        out_shape=jax.ShapeDtypeStruct((piece_rows, LANES), F32),
        in_specs=[VMEM],
        out_specs=VMEM,
    )(arrived)
    whole = exchanged(piece, "ex_0")
    copies = jnp.broadcast_to(whole[None], (near, piece_rows, LANES)).reshape(blocks * slab, LANES)
    mine = exchanged(copies, ("ex_1", "ex_2"))
    theirs = lax.ppermute(mine, "layer", swap)

    square = pltpu.VMEM((width, width), F32)
    solved, score = pl.pallas_call(
        functools.partial(solve_kernel, count),
        out_shape=(
            jax.ShapeDtypeStruct((row_count, width), F32),
            jax.ShapeDtypeStruct((1, row_count), F32),
        ),
        in_specs=[SMEM, SMEM, SMEM, VMEM, VMEM, VMEM, VMEM],
        out_specs=(VMEM, VMEM),
        scratch_shapes=[square] * 9,
    )(core, damping, damp, mine, theirs, own, other)
    return solved[None], score.reshape(row_count)


def solution(mesh):
    torus = Mesh(
        mesh.devices.reshape(mesh.shape["layer"], 8, 4, 4), ("layer", "ex_0", "ex_1", "ex_2")
    )
    in_specs = (P("layer", EX, None), P(EX), P("layer"))
    out_specs = (P("layer", EX, None), P(EX))
    return jax.shard_map(
        on_device, mesh=torus, in_specs=in_specs, out_specs=out_specs, check_vma=False
    )
```

```python
import functools

import jax
import jax.numpy as jnp
from jax import lax
from jax.experimental import pallas as pl
from jax.experimental.pallas import tpu as pltpu
from jax.sharding import Mesh
from jax.sharding import PartitionSpec as P

EX = ("ex_0", "ex_1", "ex_2")
F32, BF16 = jnp.float32, jnp.bfloat16
LANES = 128
RESIDUAL = 0.008
STEPS = 60


def dot(a, b, dims=((1,), (0,)), precision=None):
    return lax.dot_general(a, b, (dims, ((), ())), preferred_element_type=F32, precision=precision)


def split(a):
    high = a.astype(BF16)
    return high, (a - high.astype(F32)).astype(BF16)


def dot_split(a, b, dims=((1,), (0,))):
    total = dot(a[0], b[0], dims)
    if len(b) > 1:
        total = total + dot(a[0], b[1], dims)
    if len(a) > 1:
        total = total + dot(a[1], b[0], dims)
    return total


def gram_kernel(width, core_ref, labeled_ref, own_ref, other_ref, out_ref):
    blocks = width // LANES
    core = core_ref[0]
    keep = (labeled_ref[...] > 0).astype(F32)
    own, other = own_ref[...], other_ref[...]
    own_t = (own.astype(F32).T * keep).astype(BF16)
    first_t = jnp.where(core == 0, own_t, (other.astype(F32).T * keep).astype(BF16))
    last = jnp.where(core == 0, other, own)
    both = jnp.concatenate([own, other], axis=1)
    slab = blocks * LANES + LANES // 2
    for i in range(blocks):
        rows = own_t[i * LANES : (i + 1) * LANES]
        product = dot(rows, both[:, i * LANES : (i + blocks) * LANES])
        for b in range(blocks):
            start = i * slab + b * LANES
            out_ref[start : start + LANES] = product[:, b * LANES : (b + 1) * LANES]
        middle = dot(first_t[i * LANES : (i + 1) * LANES], last[:, i * LANES : (i + 1) * LANES])
        start = i * slab + blocks * LANES
        half = LANES // 2
        out_ref[start : start + half] = jnp.where(core == 0, middle[:half], middle[half:])


def sum_kernel(parts, copies, in_ref, out_ref):
    rows = in_ref.shape[0] // parts
    total = in_ref[:rows]
    for part in range(1, parts):
        total = total + in_ref[part * rows : (part + 1) * rows]
    for copy in range(copies):
        out_ref[copy * rows : (copy + 1) * rows] = total


def eye(width):
    rows = lax.broadcasted_iota(jnp.int32, (width, width), 0)
    return rows == lax.broadcasted_iota(jnp.int32, (width, width), 1)


def invert(s_ref, a_ref, x_ref, r_ref):
    width = s_ref.shape[0]
    unit = eye(width)
    one = unit.astype(F32)
    diagonal = jnp.where(unit, s_ref[...], 0.0)
    scale_row = lax.rsqrt(jnp.sum(diagonal, axis=0, keepdims=True))
    scale_col = lax.rsqrt(jnp.sum(diagonal, axis=1, keepdims=True))
    a_ref[...] = s_ref[...] * scale_col * scale_row

    e = one - a_ref[...]
    e1 = e.astype(BF16)
    e2 = dot(e1, e1).astype(BF16)
    x_ref[...] = one + e
    x_ref[...] += dot(x_ref[...].astype(BF16), e2)
    e4 = dot(e2, e2)
    x_ref[...] += dot(x_ref[...].astype(BF16), e4.astype(BF16))
    contracts = jnp.sum(e4 * e4) < 0.1

    @pl.when(jnp.logical_not(contracts))
    def _():
        largest = jnp.max(jnp.sum(jnp.abs(a_ref[...]), axis=1, keepdims=True))
        x_ref[...] = jnp.where(unit, 1.0 / largest, 0.0)

    r_ref[...] = one - dot_split(split(a_ref[...]), split(x_ref[...]))

    def far(state):
        step, norm = state
        return jnp.logical_and(step < STEPS, norm > RESIDUAL**2)

    def newton(state):
        tile = width // 4

        def advance(t, _):
            at = pl.ds(pl.multiple_of(t * tile, tile), tile)
            x_ref[at, :] += dot(x_ref[at, :], r_ref[...], precision=lax.Precision.HIGHEST)
            return 0

        def residual(t, _):
            at = pl.ds(pl.multiple_of(t * tile, tile), tile)
            r_ref[at, :] = -dot(a_ref[at, :], x_ref[...], precision=lax.Precision.HIGHEST)
            return 0

        lax.fori_loop(0, 4, advance, 0)
        lax.fori_loop(0, 4, residual, 0)
        r_ref[...] += eye(width).astype(F32)
        return state[0] + 1, jnp.sum(r_ref[...] * r_ref[...])

    lax.while_loop(far, newton, (jnp.int32(0), jnp.sum(r_ref[...] * r_ref[...])))
    x_ref[...] += dot(x_ref[...].astype(BF16), r_ref[...].astype(BF16))
    x_ref[...] = x_ref[...] * scale_col * scale_row


def solve_kernel(
    count, core_ref, damp_ref, damp_other_ref, mine_ref, theirs_ref, own_ref, other_ref,
    solved_ref, score_ref, s_ref, c_ref, ct_ref, d1_ref, a_ref, x_ref, r_ref, y_ref, p0_ref,
):
    core = core_ref[0]
    width = own_ref.shape[1]
    blocks = width // LANES
    half = LANES // 2
    slab = blocks * LANES + half
    near = core == 0
    damp0 = jnp.where(near, damp_ref[0], damp_other_ref[0])
    damp1 = jnp.where(near, damp_other_ref[0], damp_ref[0])

    def part(layer, i, start, rows):
        at = i * slab + start
        mine, theirs = mine_ref[at : at + rows], theirs_ref[at : at + rows]
        first, second = (mine, theirs) if layer == 0 else (theirs, mine)
        return jnp.where(near, first, second) * (1.0 / count)

    def put(ref, i, j, block):
        ref[i * LANES : (i + 1) * LANES, j * LANES : (j + 1) * LANES] = block

    unit = eye(LANES)
    for layer, ref, damp in ((0, s_ref, damp0), (1, d1_ref, damp1)):
        for i in range(blocks):
            for b in range(blocks):
                block = part(layer, i, b * LANES, LANES)
                j = i + b
                if b == 0:
                    put(ref, i, i, block + jnp.where(unit, damp, 0.0))
                elif j < blocks:
                    put(ref, i, j, block)
                    put(ref, j, i, block.T)
                elif layer == 0:
                    put(c_ref, i, j - blocks, block)
                    put(ct_ref, j - blocks, i, block.T)
                else:
                    put(ct_ref, i, j - blocks, block)
                    put(c_ref, j - blocks, i, block.T)
    for i in range(blocks):
        block = jnp.concatenate([part(0, i, blocks * LANES, half), part(1, i, blocks * LANES, half)], 0)
        put(c_ref, i, i, block)
        put(ct_ref, i, i, block.T)

    def section(layer, _):
        invert(s_ref, a_ref, x_ref, r_ref)

        @pl.when(layer == 0)
        def _():
            p0_ref[...] = x_ref[...]
            y_ref[...] = dot_split(split(x_ref[...]), split(c_ref[...]))
            s_ref[...] = d1_ref[...] - dot_split(split(ct_ref[...]), split(y_ref[...]))

        return 0

    lax.fori_loop(0, 2, section, 0)
    own, other = own_ref[...], other_ref[...]
    g0 = jnp.where(near, own, other)
    g1 = jnp.where(near, other, own)
    y = split(y_ref[...])
    left = g1.astype(F32) - dot_split((g0,), y)
    z1 = dot_split(split(left), split(x_ref[...]))
    z0 = dot_split((g0,), split(p0_ref[...])) - dot_split(split(z1), y, ((1,), (1,)))
    solved_ref[...] = jnp.where(near, z0, z1)
    gain = g0.astype(F32) * z0 + g1.astype(F32) * z1
    penalty = damp0 * (z0 * z0) + damp1 * (z1 * z1)

    def candidate_sum(terms):
        folded = terms[:, :LANES]
        for b in range(1, blocks):
            folded = folded + terms[:, b * LANES : (b + 1) * LANES]
        return jnp.sum(folded.T, axis=0, keepdims=True)

    gain, penalty = candidate_sum(gain), candidate_sum(penalty)
    score_ref[...] = (gain - penalty) / (1.0 + gain)


SMEM = pl.BlockSpec(memory_space=pltpu.SMEM)
VMEM = pl.BlockSpec(memory_space=pltpu.VMEM)


def limit(mebibytes):
    return pltpu.CompilerParams(vmem_limit_bytes=mebibytes * 2**20)


def exchanged(array, axis):
    devices = lax.axis_size(axis)
    parts = lax.all_to_all(array.reshape(devices, 1, -1), axis, 0, 0, tiled=True)
    return parts.reshape(array.shape)


def on_device(grads, labeled, damping):
    _, row_count, width = grads.shape
    count = row_count * lax.axis_size(EX)
    core = lax.axis_index("layer").astype(jnp.int32).reshape(1)
    swap = [(0, 1), (1, 0)]
    own = grads[0]
    other = lax.ppermute(own, "layer", swap)
    damp = lax.ppermute(damping, "layer", swap)
    blocks = width // LANES
    slab = blocks * LANES + LANES // 2
    far, near = lax.axis_size("ex_0"), lax.axis_size(("ex_1", "ex_2"))

    piece_rows = blocks * slab // near

    products = pl.pallas_call(
        functools.partial(gram_kernel, width),
        out_shape=jax.ShapeDtypeStruct((blocks * slab, LANES), F32),
        in_specs=[SMEM, VMEM, VMEM, VMEM],
        out_specs=VMEM,
        compiler_params=limit(16),
    )(core, labeled.reshape(1, row_count), own, other)
    arrived = exchanged(products, ("ex_1", "ex_2"))
    slab_part = pl.pallas_call(
        functools.partial(sum_kernel, near, 1),
        out_shape=jax.ShapeDtypeStruct((piece_rows, LANES), F32),
        in_specs=[VMEM],
        out_specs=VMEM,
        compiler_params=limit(8),
    )(arrived)
    arrived = exchanged(slab_part, "ex_0")
    piece = pl.pallas_call(
        functools.partial(sum_kernel, far, far),
        out_shape=jax.ShapeDtypeStruct((piece_rows, LANES), F32),
        in_specs=[VMEM],
        out_specs=VMEM,
        compiler_params=limit(8),
    )(arrived)
    whole = exchanged(piece, "ex_0")
    copies = jnp.broadcast_to(whole[None], (near, piece_rows, LANES)).reshape(blocks * slab, LANES)
    mine = exchanged(copies, ("ex_1", "ex_2"))
    theirs = lax.ppermute(mine, "layer", swap)

    square = pltpu.VMEM((width, width), F32)
    solved, score = pl.pallas_call(
        functools.partial(solve_kernel, count),
        out_shape=(
            jax.ShapeDtypeStruct((row_count, width), F32),
            jax.ShapeDtypeStruct((1, row_count), F32),
        ),
        in_specs=[SMEM, SMEM, SMEM, VMEM, VMEM, VMEM, VMEM],
        out_specs=(VMEM, VMEM),
        scratch_shapes=[square] * 9,
        compiler_params=limit(32),
    )(core, damping, damp, mine, theirs, own, other)
    return solved[None], score.reshape(row_count)


def solution(mesh):
    torus = Mesh(
        mesh.devices.reshape(mesh.shape["layer"], 8, 4, 4), ("layer", "ex_0", "ex_1", "ex_2")
    )
    in_specs = (P("layer", EX, None), P(EX), P("layer"))
    out_specs = (P("layer", EX, None), P(EX))
    return jax.shard_map(
        on_device, mesh=torus, in_specs=in_specs, out_specs=out_specs, check_vma=False
    )
```

```python
import functools

import jax
import jax.numpy as jnp
from jax import lax
from jax.experimental import pallas as pl
from jax.experimental.pallas import tpu as pltpu
from jax.sharding import Mesh
from jax.sharding import PartitionSpec as P

EX = ("z_hi", "z_lo", "y", "x")
FAR, NEAR = EX[0], EX[1:]
F32, BF16 = jnp.float32, jnp.bfloat16
LANES = 128
RESIDUAL = 0.008
STEPS = 60


def dot(a, b, dims=((1,), (0,)), precision=None):
    return lax.dot_general(a, b, (dims, ((), ())), preferred_element_type=F32, precision=precision)


def split(a):
    high = a.astype(BF16)
    return high, (a - high.astype(F32)).astype(BF16)


def dot_split(a, b, dims=((1,), (0,))):
    total = dot(a[0], b[0], dims)
    if len(b) > 1:
        total = total + dot(a[0], b[1], dims)
    if len(a) > 1:
        total = total + dot(a[1], b[0], dims)
    return total


def gram_kernel(width, core_ref, labeled_ref, own_ref, other_ref, out_ref):
    blocks = width // LANES
    core = core_ref[0]
    keep = (labeled_ref[...] > 0).astype(F32)
    own, other = own_ref[...], other_ref[...]
    own_t = (own.astype(F32).T * keep).astype(BF16)
    first_t = jnp.where(core == 0, own_t, (other.astype(F32).T * keep).astype(BF16))
    last = jnp.where(core == 0, other, own)
    both = jnp.concatenate([own, other], axis=1)
    slab = blocks * LANES + LANES // 2
    for i in range(blocks):
        rows = own_t[i * LANES : (i + 1) * LANES]
        product = dot(rows, both[:, i * LANES : (i + blocks) * LANES])
        for b in range(blocks):
            start = i * slab + b * LANES
            out_ref[start : start + LANES] = product[:, b * LANES : (b + 1) * LANES]
        middle = dot(first_t[i * LANES : (i + 1) * LANES], last[:, i * LANES : (i + 1) * LANES])
        start = i * slab + blocks * LANES
        half = LANES // 2
        out_ref[start : start + half] = jnp.where(core == 0, middle[:half], middle[half:])


def sum_kernel(parts, copies, in_ref, out_ref):
    rows = in_ref.shape[0] // parts
    total = in_ref[:rows]
    for part in range(1, parts):
        total = total + in_ref[part * rows : (part + 1) * rows]
    for copy in range(copies):
        out_ref[copy * rows : (copy + 1) * rows] = total


def eye(width):
    rows = lax.broadcasted_iota(jnp.int32, (width, width), 0)
    return rows == lax.broadcasted_iota(jnp.int32, (width, width), 1)


def invert(s_ref, a_ref, x_ref, r_ref):
    width = s_ref.shape[0]
    unit = eye(width)
    one = unit.astype(F32)
    diagonal = jnp.where(unit, s_ref[...], 0.0)
    scale_row = lax.rsqrt(jnp.sum(diagonal, axis=0, keepdims=True))
    scale_col = lax.rsqrt(jnp.sum(diagonal, axis=1, keepdims=True))
    a_ref[...] = s_ref[...] * scale_col * scale_row

    e = one - a_ref[...]
    e1 = e.astype(BF16)
    e2 = dot(e1, e1).astype(BF16)
    x_ref[...] = one + e
    x_ref[...] += dot(x_ref[...].astype(BF16), e2)
    e4 = dot(e2, e2)
    x_ref[...] += dot(x_ref[...].astype(BF16), e4.astype(BF16))
    contracts = jnp.sum(e4 * e4) < 0.1

    @pl.when(jnp.logical_not(contracts))
    def _():
        largest = jnp.max(jnp.sum(jnp.abs(a_ref[...]), axis=1, keepdims=True))
        x_ref[...] = jnp.where(unit, 1.0 / largest, 0.0)

    r_ref[...] = one - dot_split(split(a_ref[...]), split(x_ref[...]))

    def far(state):
        step, norm = state
        return jnp.logical_and(step < STEPS, norm > RESIDUAL**2)

    def newton(state):
        tile = width // 4

        def advance(t, _):
            at = pl.ds(pl.multiple_of(t * tile, tile), tile)
            x_ref[at, :] += dot(x_ref[at, :], r_ref[...], precision=lax.Precision.HIGHEST)
            return 0

        def residual(t, _):
            at = pl.ds(pl.multiple_of(t * tile, tile), tile)
            r_ref[at, :] = -dot(a_ref[at, :], x_ref[...], precision=lax.Precision.HIGHEST)
            return 0

        lax.fori_loop(0, 4, advance, 0)
        lax.fori_loop(0, 4, residual, 0)
        r_ref[...] += eye(width).astype(F32)
        return state[0] + 1, jnp.sum(r_ref[...] * r_ref[...])

    lax.while_loop(far, newton, (jnp.int32(0), jnp.sum(r_ref[...] * r_ref[...])))
    x_ref[...] += dot(x_ref[...].astype(BF16), r_ref[...].astype(BF16))
    x_ref[...] = x_ref[...] * scale_col * scale_row


def solve_kernel(
    count, core_ref, damp_ref, damp_other_ref, mine_ref, theirs_ref, own_ref, other_ref,
    solved_ref, score_ref, s_ref, c_ref, ct_ref, d1_ref, a_ref, x_ref, r_ref, y_ref, p0_ref,
):
    core = core_ref[0]
    width = own_ref.shape[1]
    blocks = width // LANES
    half = LANES // 2
    slab = blocks * LANES + half
    near = core == 0
    damp0 = jnp.where(near, damp_ref[0], damp_other_ref[0])
    damp1 = jnp.where(near, damp_other_ref[0], damp_ref[0])

    def part(layer, i, start, rows):
        at = i * slab + start
        mine, theirs = mine_ref[at : at + rows], theirs_ref[at : at + rows]
        first, second = (mine, theirs) if layer == 0 else (theirs, mine)
        return jnp.where(near, first, second) * (1.0 / count)

    def put(ref, i, j, block):
        ref[i * LANES : (i + 1) * LANES, j * LANES : (j + 1) * LANES] = block

    unit = eye(LANES)
    for layer, ref, damp in ((0, s_ref, damp0), (1, d1_ref, damp1)):
        for i in range(blocks):
            for b in range(blocks):
                block = part(layer, i, b * LANES, LANES)
                j = i + b
                if b == 0:
                    put(ref, i, i, block + jnp.where(unit, damp, 0.0))
                elif j < blocks:
                    put(ref, i, j, block)
                    put(ref, j, i, block.T)
                elif layer == 0:
                    put(c_ref, i, j - blocks, block)
                    put(ct_ref, j - blocks, i, block.T)
                else:
                    put(ct_ref, i, j - blocks, block)
                    put(c_ref, j - blocks, i, block.T)
    for i in range(blocks):
        block = jnp.concatenate([part(0, i, blocks * LANES, half), part(1, i, blocks * LANES, half)], 0)
        put(c_ref, i, i, block)
        put(ct_ref, i, i, block.T)

    def section(layer, _):
        invert(s_ref, a_ref, x_ref, r_ref)

        @pl.when(layer == 0)
        def _():
            p0_ref[...] = x_ref[...]
            y_ref[...] = dot_split(split(x_ref[...]), split(c_ref[...]))
            s_ref[...] = d1_ref[...] - dot_split(split(ct_ref[...]), split(y_ref[...]))

        return 0

    lax.fori_loop(0, 2, section, 0)
    own, other = own_ref[...], other_ref[...]
    g0 = jnp.where(near, own, other)
    g1 = jnp.where(near, other, own)
    y = split(y_ref[...])
    left = g1.astype(F32) - dot_split((g0,), y)
    z1 = dot_split(split(left), split(x_ref[...]))
    z0 = dot_split((g0,), split(p0_ref[...])) - dot_split(split(z1), y, ((1,), (1,)))
    solved_ref[...] = jnp.where(near, z0, z1)
    gain = g0.astype(F32) * z0 + g1.astype(F32) * z1
    penalty = damp0 * (z0 * z0) + damp1 * (z1 * z1)

    def candidate_sum(terms):
        folded = terms[:, :LANES]
        for b in range(1, blocks):
            folded = folded + terms[:, b * LANES : (b + 1) * LANES]
        return jnp.sum(folded.T, axis=0, keepdims=True)

    gain, penalty = candidate_sum(gain), candidate_sum(penalty)
    score_ref[...] = (gain - penalty) / (1.0 + gain)


SMEM = pl.BlockSpec(memory_space=pltpu.SMEM)
VMEM = pl.BlockSpec(memory_space=pltpu.VMEM)


def limit(mebibytes):
    return pltpu.CompilerParams(vmem_limit_bytes=mebibytes * 2**20)


def exchanged(array, axis):
    devices = lax.axis_size(axis)
    parts = lax.all_to_all(array.reshape(devices, 1, -1), axis, 0, 0, tiled=True)
    return parts.reshape(array.shape)


def summed(array, parts, copies):
    rows = array.shape[0] // parts
    return pl.pallas_call(
        functools.partial(sum_kernel, parts, copies),
        out_shape=jax.ShapeDtypeStruct((copies * rows, LANES), F32),
        in_specs=[VMEM],
        out_specs=VMEM,
        compiler_params=limit(8),
    )(array)


def on_device(grads, labeled, damping):
    _, row_count, width = grads.shape
    count = row_count * lax.axis_size(EX)
    core = lax.axis_index("layer").astype(jnp.int32).reshape(1)
    swap = [(0, 1), (1, 0)]
    own = grads[0]
    other = lax.ppermute(own, "layer", swap)
    damp = lax.ppermute(damping, "layer", swap)
    blocks = width // LANES
    slab = blocks * LANES + LANES // 2
    pieces, planes = lax.axis_size(NEAR), lax.axis_size(FAR)
    products = pl.pallas_call(
        functools.partial(gram_kernel, width),
        out_shape=jax.ShapeDtypeStruct((blocks * slab, LANES), F32),
        in_specs=[SMEM, VMEM, VMEM, VMEM],
        out_specs=VMEM,
        compiler_params=limit(16),
    )(core, labeled.reshape(1, row_count), own, other)
    partial = summed(exchanged(products, NEAR), pieces, planes)
    total = summed(exchanged(partial, FAR), planes, pieces)
    mine = exchanged(total, NEAR)
    theirs = lax.ppermute(mine, "layer", swap)

    square = pltpu.VMEM((width, width), F32)
    solved, score = pl.pallas_call(
        functools.partial(solve_kernel, count),
        out_shape=(
            jax.ShapeDtypeStruct((row_count, width), F32),
            jax.ShapeDtypeStruct((1, row_count), F32),
        ),
        in_specs=[SMEM, SMEM, SMEM, VMEM, VMEM, VMEM, VMEM],
        out_specs=(VMEM, VMEM),
        scratch_shapes=[square] * 9,
        compiler_params=limit(32),
    )(core, damping, damp, mine, theirs, own, other)
    return solved[None], score.reshape(row_count)


def solution(mesh):
    torus = Mesh(
        mesh.devices.reshape(mesh.shape["layer"], 4, 2, 4, 4), ("layer", *EX)
    )
    in_specs = (P("layer", EX, None), P(EX), P("layer"))
    out_specs = (P("layer", EX, None), P(EX))
    return jax.shard_map(
        on_device, mesh=torus, in_specs=in_specs, out_specs=out_specs, check_vma=False
    )
```

```python
import functools

import jax
import jax.numpy as jnp
from jax import lax
from jax.experimental import pallas as pl
from jax.experimental.pallas import tpu as pltpu
from jax.sharding import Mesh
from jax.sharding import PartitionSpec as P

EX = ("z_hi", "z_lo", "y", "x")
FAR, NEAR = EX[0], EX[1:]
F32, BF16 = jnp.float32, jnp.bfloat16
LANES = 128
HALF = LANES // 2
RESIDUAL = 0.002
STEPS = 60
TILES = 4
REFINEMENTS = 3


def dot(a, b, dims=((1,), (0,)), precision=None):
    return lax.dot_general(a, b, (dims, ((), ())), preferred_element_type=F32, precision=precision)


def split(a):
    high = a.astype(BF16)
    return high, (a - high.astype(F32)).astype(BF16)


def dot_split(a, b, dims=((1,), (0,))):
    total = dot(a[0], b[0], dims)
    if len(b) > 1:
        total = total + dot(a[0], b[1], dims)
    if len(a) > 1:
        total = total + dot(a[1], b[0], dims)
    return total


def dot_full(out_ref, a_ref, b, base_ref=None, dims=((1,), (0,))):
    tile = a_ref.shape[0] // TILES

    def step(t, _):
        at = pl.ds(pl.multiple_of(t * tile, tile), tile)
        product = dot(a_ref[at, :].astype(F32), b[...], dims, lax.Precision.HIGHEST)
        out_ref[at, :] = product if base_ref is None else base_ref[at, :].astype(F32) - product
        return 0

    lax.fori_loop(0, TILES, step, 0)


def mask_kernel(labeled_ref, own_ref, out_ref):
    keep = (labeled_ref[...] > 0).astype(F32)
    out_ref[...] = (own_ref[...].astype(F32).T * keep).astype(BF16)


def gram_kernel(core_ref, labeled_ref, own_t_ref, own_ref, other_ref, out_ref):
    core = core_ref[0]
    keep = (labeled_ref[...] > 0).astype(F32)
    own_t, own, other = own_t_ref[...], own_ref[...], other_ref[...]
    blocks = own.shape[1] // LANES
    first_t = jnp.where(core == 0, own_t, (other.astype(F32).T * keep).astype(BF16))
    last = jnp.where(core == 0, other, own)
    both = jnp.concatenate([own, other], axis=1)
    slab = blocks * LANES + HALF
    for i in range(blocks):
        rows = own_t[i * LANES : (i + 1) * LANES]
        product = dot(rows, both[:, i * LANES : (i + blocks) * LANES])
        for b in range(blocks):
            start = i * slab + b * LANES
            out_ref[start : start + LANES] = product[:, b * LANES : (b + 1) * LANES]
        middle = dot(first_t[i * LANES : (i + 1) * LANES], last[:, i * LANES : (i + 1) * LANES])
        start = i * slab + blocks * LANES
        out_ref[start : start + HALF] = jnp.where(core == 0, middle[:HALF], middle[HALF:])


def sum_kernel(in_ref, out_ref):
    rows = out_ref.shape[0]
    total = in_ref[:rows]
    for part in range(1, in_ref.shape[0] // rows):
        total = total + in_ref[part * rows : (part + 1) * rows]
    out_ref[...] = total


def total_kernel(*refs):
    out_ref = refs[-1]
    total = refs[0][...]
    for ref in refs[1:-1]:
        total = total + ref[...]
    rows = total.shape[0]
    for copy in range(out_ref.shape[0] // rows):
        out_ref[copy * rows : (copy + 1) * rows] = total


def eye(width):
    rows = lax.broadcasted_iota(jnp.int32, (width, width), 0)
    return rows == lax.broadcasted_iota(jnp.int32, (width, width), 1)


def invert(s_ref, a_ref, x_ref, r_ref, t_ref, refresh=None, known_hard=None):
    width = s_ref.shape[0]

    def scales():
        diagonal = jnp.where(eye(width), s_ref[...], 0.0)
        row = lax.rsqrt(jnp.sum(diagonal, axis=0, keepdims=True))
        return lax.rsqrt(jnp.sum(diagonal, axis=1, keepdims=True)), row

    def scaled():
        column, row = scales()
        a_ref[...] = s_ref[...] * column * row

    def square():
        r = r_ref[...].astype(BF16)
        t = dot(r, r)
        t_ref[...] = t
        return jnp.sum(t * t)

    def residual():
        dot_full(r_ref, a_ref, x_ref)
        r_ref[...] = eye(width).astype(F32) - r_ref[...]

    scaled()
    one = eye(width).astype(F32)
    e = one - a_ref[...]
    e1 = e.astype(BF16)
    e2 = dot(e1, e1).astype(BF16)
    x = one + e
    x_ref[...] = x + dot(x.astype(BF16), e2)
    r_ref[...] = one - dot_split(split(a_ref[...]), split(x_ref[...]))
    norm = square()
    hard = jnp.logical_not(norm <= RESIDUAL**2)
    if known_hard is not None:
        hard = jnp.logical_or(hard, known_hard)

    @pl.when(hard)
    def _():
        if refresh is not None:
            refresh()
        scaled()

        @pl.when(jnp.logical_not(norm < 0.25))
        def _():
            largest = jnp.max(jnp.sum(jnp.abs(a_ref[...]), axis=1, keepdims=True))
            x_ref[...] = jnp.where(eye(width), 1.0 / largest, 0.0)

        residual()

        def far(state):
            return jnp.logical_and(state[0] < STEPS, state[1] > 0.01 * RESIDUAL**2)

        def newton(state):
            dot_full(t_ref, x_ref, r_ref)
            x_ref[...] += t_ref[...]
            residual()
            return state[0] + 1, square()

        lax.while_loop(far, newton, (jnp.int32(0), square()))

    step = (r_ref[...] + t_ref[...]).astype(BF16)
    column, row = scales()
    x_ref[...] = (x_ref[...] + dot(x_ref[...].astype(BF16), step)) * column * row
    return hard


def part(ref, i, start, rows, blocks, count):
    at = i * (blocks * LANES + HALF) + start
    return ref[at : at + rows] * (1.0 / count)


def put(ref, i, j, block):
    ref[i * LANES : (i + 1) * LANES, j * LANES : (j + 1) * LANES] = block


def put_diagonal(ref, slabs_ref, damp, count):
    blocks = ref.shape[0] // LANES
    unit = eye(LANES)
    for i in range(blocks):
        put(ref, i, i, part(slabs_ref, i, 0, LANES, blocks, count) + jnp.where(unit, damp, 0.0))
        for j in range(i + 1, blocks):
            block = part(slabs_ref, i, (j - i) * LANES, LANES, blocks, count)
            put(ref, i, j, block)
            put(ref, j, i, block.T)


def first_kernel(count, damp_ref, mine_ref, x_ref, hard_ref, s_ref, a_ref, r_ref, t_ref):
    put_diagonal(s_ref, mine_ref, damp_ref[0], count)
    hard_ref[0] = invert(s_ref, a_ref, x_ref, r_ref, t_ref).astype(jnp.int32)


def solve_kernel(
    count, core_ref, hard_ref, damp_ref, damp_other_ref, mine_ref, theirs_ref, first_ref, own_ref,
    other_ref, solved_ref, score_ref, s_ref, d_ref, c_ref, ct_ref, a_ref, x_ref, r_ref, t_ref, y_ref,
    left_ref,
):
    near = core_ref[0] == 0
    width = own_ref.shape[1]
    blocks = width // LANES
    damp, damp_other = damp_ref[0], damp_other_ref[0]

    for i in range(blocks):
        for j in range(i):
            start = (j + blocks - i) * LANES
            block = part(mine_ref, i, start, LANES, blocks, count)
            put(c_ref, i, j, block)
            put(ct_ref, j, i, block.T)
            block = part(theirs_ref, i, start, LANES, blocks, count)
            put(ct_ref, i, j, block)
            put(c_ref, j, i, block.T)
        mine = part(mine_ref, i, blocks * LANES, HALF, blocks, count)
        theirs = part(theirs_ref, i, blocks * LANES, HALF, blocks, count)
        block = jnp.concatenate([jnp.where(near, mine, theirs), jnp.where(near, theirs, mine)], 0)
        turned = block.T
        put(c_ref, i, i, jnp.where(near, block, turned))
        put(ct_ref, i, i, jnp.where(near, turned, block))
    put_diagonal(d_ref, theirs_ref, damp_other, count)

    first = split(first_ref[...])
    y_ref[...] = dot_split(first, split(c_ref[...]))
    s_ref[...] = d_ref[...] - dot_split(split(ct_ref[...]), split(y_ref[...]))

    def refresh():
        dot_full(y_ref, first_ref, c_ref)
        dot_full(s_ref, ct_ref, y_ref, d_ref)

    hard = invert(s_ref, a_ref, x_ref, r_ref, t_ref, refresh, hard_ref[0] > 0)

    def outputs(z_own, z_other):
        solved_ref[...] = z_own
        gain = own_ref[...].astype(F32) * z_own + other_ref[...].astype(F32) * z_other
        penalty = damp * (z_own * z_own) + damp_other * (z_other * z_other)

        def candidate_sum(terms):
            folded = terms[:, :LANES]
            for b in range(1, blocks):
                folded = folded + terms[:, b * LANES : (b + 1) * LANES]
            return jnp.sum(folded.T, axis=0, keepdims=True)

        gain, penalty = candidate_sum(gain), candidate_sum(penalty)
        score_ref[...] = (gain - penalty) / (1.0 + gain)

    @pl.when(hard)
    def _():
        count_rows = left_ref.shape[0]
        top, bottom = pl.ds(0, count_rows), pl.ds(count_rows, count_rows)
        z_own, z_other = a_ref.at[top], a_ref.at[bottom]
        rest_own, rest_other = r_ref.at[top], r_ref.at[bottom]
        step_own, step_other = t_ref.at[top], t_ref.at[bottom]
        put_diagonal(s_ref, mine_ref, damp, count)
        a_ref[...] = jnp.zeros_like(a_ref)
        rest_own[...] = own_ref[...].astype(F32)
        rest_other[...] = other_ref[...].astype(F32)

        def refine(_, carry):
            dot_full(left_ref, rest_own, y_ref, rest_other)
            dot_full(step_other, left_ref, x_ref)
            dot_full(left_ref, rest_own, first_ref)
            dot_full(step_own, step_other, y_ref, left_ref, ((1,), (1,)))
            a_ref[...] += t_ref[...]
            dot_full(left_ref, z_own, s_ref, own_ref)
            dot_full(rest_own, z_other, ct_ref, left_ref)
            dot_full(left_ref, z_own, c_ref, other_ref)
            dot_full(rest_other, z_other, d_ref, left_ref)
            return carry

        lax.fori_loop(0, REFINEMENTS, refine, 0)
        outputs(z_own[...], z_other[...])

    @pl.when(jnp.logical_not(hard))
    def _():
        own = (own_ref[...],)
        y = split(y_ref[...])
        left = other_ref[...].astype(F32) - dot_split(own, y)
        z_other = dot_split(split(left), split(x_ref[...]))
        z_own = dot_split(own, split(first_ref[...])) - dot_split(split(z_other), y, ((1,), (1,)))
        outputs(z_own, z_other)


SMEM = pl.BlockSpec(memory_space=pltpu.SMEM)
VMEM = pl.BlockSpec(memory_space=pltpu.VMEM)


def call(kernel, out_shape, in_specs, mebibytes, megaflops=0, out_specs=VMEM, scratch=()):
    return pl.pallas_call(
        kernel,
        out_shape=out_shape,
        in_specs=in_specs,
        out_specs=out_specs,
        scratch_shapes=scratch,
        compiler_params=pltpu.CompilerParams(vmem_limit_bytes=mebibytes * 2**20),
        cost_estimate=pl.CostEstimate(
            flops=megaflops * 10**6, bytes_accessed=2**20, transcendentals=0
        ),
    )


def exchanged(array, axis):
    devices = lax.axis_size(axis)
    parts = lax.all_to_all(array.reshape(devices, 1, -1), axis, 0, 0, tiled=True)
    return parts.reshape(array.shape)


def from_others(array, axis):
    devices = lax.axis_size(axis)
    return [
        lax.ppermute(array, axis, [(i, (i + shift) % devices) for i in range(devices)])
        for shift in range(1, devices)
    ]


def on_device(grads, labeled, damping):
    _, row_count, width = grads.shape
    count = row_count * lax.axis_size(EX)
    core = lax.axis_index("layer").astype(jnp.int32).reshape(1)
    swap = [(0, 1), (1, 0)]
    own = grads[0]
    labeled = labeled.reshape(1, row_count)
    other = lax.ppermute(own, "layer", swap)
    damping_other = lax.ppermute(damping, "layer", swap)
    blocks = width // LANES
    rows = blocks * (blocks * LANES + HALF)
    pieces, planes = lax.axis_size(NEAR), lax.axis_size(FAR)
    square = pltpu.VMEM((width, width), F32)
    matrix = jax.ShapeDtypeStruct((width, width), F32)

    def slabs(length):
        return jax.ShapeDtypeStruct((length, LANES), F32)

    own_t = call(mask_kernel, jax.ShapeDtypeStruct((width, row_count), BF16), [VMEM] * 2, 8, 500)(
        labeled, own
    )
    products = call(gram_kernel, slabs(rows), [SMEM] + [VMEM] * 4, 16, 500)(
        core, labeled, own_t, own, other
    )
    partial = call(sum_kernel, slabs(rows // pieces), [VMEM], 8, 50)(exchanged(products, NEAR))
    partials = [partial, *from_others(partial, FAR)]
    total = call(total_kernel, slabs(rows), [VMEM] * planes, 8, 50)(*partials)
    mine = exchanged(total, NEAR)
    theirs = lax.ppermute(mine, "layer", swap)
    first, hard = call(
        functools.partial(first_kernel, count),
        (matrix, jax.ShapeDtypeStruct((1,), jnp.int32)),
        [SMEM, VMEM],
        16,
        3000,
        (VMEM, SMEM),
        [square] * 4,
    )(damping, mine)
    solved, score = call(
        functools.partial(solve_kernel, count),
        (
            jax.ShapeDtypeStruct((row_count, width), F32),
            jax.ShapeDtypeStruct((1, row_count), F32),
        ),
        [SMEM] * 4 + [VMEM] * 5,
        32,
        6000,
        (VMEM, VMEM),
        [square] * 9 + [pltpu.VMEM((row_count, width), F32)],
    )(core, hard, damping, damping_other, mine, theirs, first, own, other)
    return solved[None], score.reshape(row_count)


def solution(mesh):
    torus = Mesh(mesh.devices.reshape(mesh.shape["layer"], 4, 2, 4, 4), ("layer", *EX))
    in_specs = (P("layer", EX, None), P(EX), P("layer"))
    out_specs = (P("layer", EX, None), P(EX))
    return jax.shard_map(
        on_device, mesh=torus, in_specs=in_specs, out_specs=out_specs, check_vma=False
    )
```

```python
import functools

import jax
import jax.numpy as jnp
from jax import lax
from jax.experimental import pallas as pl
from jax.experimental.pallas import tpu as pltpu
from jax.sharding import Mesh
from jax.sharding import PartitionSpec as P

EX = ("z_hi", "z_lo", "y", "x")
FAR, PAIR, SHEET, NEAR = EX[0], EX[1], EX[2:], EX[1:]
F32, BF16 = jnp.float32, jnp.bfloat16
LANES = 128
HALF = LANES // 2
RESIDUAL = 0.002
STEPS = 60
TILES = 4
REFINEMENTS = 3


def dot(a, b, dims=((1,), (0,)), precision=None):
    return lax.dot_general(a, b, (dims, ((), ())), preferred_element_type=F32, precision=precision)


def split(a):
    high = a.astype(BF16)
    return high, (a - high.astype(F32)).astype(BF16)


def dot_split(a, b, dims=((1,), (0,))):
    total = dot(a[0], b[0], dims)
    if len(b) > 1:
        total = total + dot(a[0], b[1], dims)
    if len(a) > 1:
        total = total + dot(a[1], b[0], dims)
    return total


def dot_full(out_ref, a_ref, b, base_ref=None, dims=((1,), (0,))):
    tile = a_ref.shape[0] // TILES

    def step(t, _):
        at = pl.ds(pl.multiple_of(t * tile, tile), tile)
        product = dot(a_ref[at, :].astype(F32), b[...], dims, lax.Precision.HIGHEST)
        out_ref[at, :] = product if base_ref is None else base_ref[at, :].astype(F32) - product
        return 0

    lax.fori_loop(0, TILES, step, 0)


def masked_turned(rows, labeled):
    return (rows.astype(F32).T * (labeled > 0).astype(F32)).astype(BF16)


def mask_kernel(labeled_ref, own_ref, other_ref, own_t_ref, other_t_ref):
    own_t_ref[...] = masked_turned(own_ref[...], labeled_ref[...])
    other_t_ref[...] = masked_turned(other_ref[...], labeled_ref[...])


def gram_kernel(
    place_ref, _, labeled_ref, own_t_ref, other_t_ref, pair_ref, pair_other_ref, out_ref, turned_ref
):
    core, side = place_ref[0], place_ref[1]
    width, rows = own_t_ref.shape
    blocks = width // LANES
    turned_ref[:width, :rows] = own_t_ref[...]
    turned_ref[width:, :rows] = other_t_ref[...]
    turned_ref[:width, rows:] = masked_turned(pair_ref[...], labeled_ref[...])
    turned_ref[width:, rows:] = masked_turned(pair_other_ref[...], labeled_ref[...])
    slab = blocks * LANES + HALF
    across = ((1,), (1,))

    def at(start, size):
        return turned_ref[pl.ds(pl.multiple_of(start, HALF), size), :]

    for k in range(blocks // 2):
        start = (side * (blocks // 2) + k) * LANES
        product = dot(at(start, LANES), at(start, width), across)
        for b in range(blocks):
            out = k * slab + b * LANES
            out_ref[out : out + LANES] = product[:, b * LANES : (b + 1) * LANES]
        layer = core * width
        middle = dot(at(start + layer + core * HALF, HALF), at(start + width - layer, LANES), across)
        out = k * slab + blocks * LANES
        out_ref[out : out + HALF] = middle


def sum_kernel(in_ref, out_ref):
    rows = out_ref.shape[0]
    total = in_ref[:rows]
    for part in range(1, in_ref.shape[0] // rows):
        total = total + in_ref[part * rows : (part + 1) * rows]
    out_ref[...] = total


def total_kernel(*refs):
    out_ref = refs[-1]
    total = refs[0][...]
    for ref in refs[1:-1]:
        total = total + ref[...]
    rows = total.shape[0]
    for copy in range(out_ref.shape[0] // rows):
        out_ref[copy * rows : (copy + 1) * rows] = total


def eye(width):
    rows = lax.broadcasted_iota(jnp.int32, (width, width), 0)
    return rows == lax.broadcasted_iota(jnp.int32, (width, width), 1)


def invert(s_ref, a_ref, x_ref, r_ref, t_ref, refresh=None, known_hard=None):
    width = s_ref.shape[0]

    def scales():
        diagonal = jnp.where(eye(width), s_ref[...], 0.0)
        row = lax.rsqrt(jnp.sum(diagonal, axis=0, keepdims=True))
        return lax.rsqrt(jnp.sum(diagonal, axis=1, keepdims=True)), row

    def scaled():
        column, row = scales()
        a_ref[...] = s_ref[...] * column * row

    def square():
        r = r_ref[...].astype(BF16)
        t = dot(r, r)
        t_ref[...] = t
        return jnp.sum(t * t)

    def residual():
        dot_full(r_ref, a_ref, x_ref)
        r_ref[...] = eye(width).astype(F32) - r_ref[...]

    scaled()
    one = eye(width).astype(F32)
    e = one - a_ref[...]
    e1 = e.astype(BF16)
    e2 = dot(e1, e1).astype(BF16)
    x = one + e
    x_ref[...] = x + dot(x.astype(BF16), e2)
    r_ref[...] = one - dot_split(split(a_ref[...]), split(x_ref[...]))
    norm = square()
    hard = jnp.logical_not(norm <= RESIDUAL**2)
    if known_hard is not None:
        hard = jnp.logical_or(hard, known_hard)

    @pl.when(hard)
    def _():
        if refresh is not None:
            refresh()
        scaled()

        @pl.when(jnp.logical_not(norm < 0.25))
        def _():
            largest = jnp.max(jnp.sum(jnp.abs(a_ref[...]), axis=1, keepdims=True))
            x_ref[...] = jnp.where(eye(width), 1.0 / largest, 0.0)

        residual()

        def far(state):
            return jnp.logical_and(state[0] < STEPS, state[1] > 0.01 * RESIDUAL**2)

        def newton(state):
            dot_full(t_ref, x_ref, r_ref)
            x_ref[...] += t_ref[...]
            residual()
            return state[0] + 1, square()

        lax.while_loop(far, newton, (jnp.int32(0), square()))

    step = (r_ref[...] + t_ref[...]).astype(BF16)
    column, row = scales()
    x_ref[...] = (x_ref[...] + dot(x_ref[...].astype(BF16), step)) * column * row
    return hard


def part(ref, i, start, rows, blocks, count):
    at = i * (blocks * LANES + HALF) + start
    return ref[at : at + rows] * (1.0 / count)


def put(ref, i, j, block):
    ref[i * LANES : (i + 1) * LANES, j * LANES : (j + 1) * LANES] = block


def put_diagonal(ref, slabs_ref, damp, count):
    blocks = ref.shape[0] // LANES
    unit = eye(LANES)
    for i in range(blocks):
        put(ref, i, i, part(slabs_ref, i, 0, LANES, blocks, count) + jnp.where(unit, damp, 0.0))
        for j in range(i + 1, blocks):
            block = part(slabs_ref, i, (j - i) * LANES, LANES, blocks, count)
            put(ref, i, j, block)
            put(ref, j, i, block.T)


def first_kernel(count, damp_ref, mine_ref, x_ref, hard_ref, s_ref, a_ref, r_ref, t_ref):
    put_diagonal(s_ref, mine_ref, damp_ref[0], count)
    hard_ref[0] = invert(s_ref, a_ref, x_ref, r_ref, t_ref).astype(jnp.int32)


def solve_kernel(
    count, core_ref, hard_ref, damp_ref, damp_other_ref, mine_ref, theirs_ref, first_ref, own_ref,
    other_ref, solved_ref, score_ref, s_ref, d_ref, c_ref, ct_ref, a_ref, x_ref, r_ref, t_ref, y_ref,
    left_ref,
):
    near = core_ref[0] == 0
    width = own_ref.shape[1]
    blocks = width // LANES
    damp, damp_other = damp_ref[0], damp_other_ref[0]

    for i in range(blocks):
        for j in range(i):
            start = (j + blocks - i) * LANES
            block = part(mine_ref, i, start, LANES, blocks, count)
            put(c_ref, i, j, block)
            put(ct_ref, j, i, block.T)
            block = part(theirs_ref, i, start, LANES, blocks, count)
            put(ct_ref, i, j, block)
            put(c_ref, j, i, block.T)
        mine = part(mine_ref, i, blocks * LANES, HALF, blocks, count)
        theirs = part(theirs_ref, i, blocks * LANES, HALF, blocks, count)
        block = jnp.concatenate([jnp.where(near, mine, theirs), jnp.where(near, theirs, mine)], 0)
        turned = block.T
        put(c_ref, i, i, jnp.where(near, block, turned))
        put(ct_ref, i, i, jnp.where(near, turned, block))
    put_diagonal(d_ref, theirs_ref, damp_other, count)

    first = split(first_ref[...])
    y_ref[...] = dot_split(first, split(c_ref[...]))
    s_ref[...] = d_ref[...] - dot_split(split(ct_ref[...]), split(y_ref[...]))

    def refresh():
        dot_full(y_ref, first_ref, c_ref)
        dot_full(s_ref, ct_ref, y_ref, d_ref)

    hard = invert(s_ref, a_ref, x_ref, r_ref, t_ref, refresh, hard_ref[0] > 0)

    def outputs(z_own, z_other):
        solved_ref[...] = z_own
        gain = own_ref[...].astype(F32) * z_own + other_ref[...].astype(F32) * z_other
        penalty = damp * (z_own * z_own) + damp_other * (z_other * z_other)

        def candidate_sum(terms):
            folded = terms[:, :LANES]
            for b in range(1, blocks):
                folded = folded + terms[:, b * LANES : (b + 1) * LANES]
            return jnp.sum(folded.T, axis=0, keepdims=True)

        gain, penalty = candidate_sum(gain), candidate_sum(penalty)
        score_ref[...] = (gain - penalty) / (1.0 + gain)

    @pl.when(hard)
    def _():
        count_rows = left_ref.shape[0]
        top, bottom = pl.ds(0, count_rows), pl.ds(count_rows, count_rows)
        z_own, z_other = a_ref.at[top], a_ref.at[bottom]
        rest_own, rest_other = r_ref.at[top], r_ref.at[bottom]
        step_own, step_other = t_ref.at[top], t_ref.at[bottom]
        put_diagonal(s_ref, mine_ref, damp, count)
        a_ref[...] = jnp.zeros_like(a_ref)
        rest_own[...] = own_ref[...].astype(F32)
        rest_other[...] = other_ref[...].astype(F32)

        def refine(_, carry):
            dot_full(left_ref, rest_own, y_ref, rest_other)
            dot_full(step_other, left_ref, x_ref)
            dot_full(left_ref, rest_own, first_ref)
            dot_full(step_own, step_other, y_ref, left_ref, ((1,), (1,)))
            a_ref[...] += t_ref[...]
            dot_full(left_ref, z_own, s_ref, own_ref)
            dot_full(rest_own, z_other, ct_ref, left_ref)
            dot_full(left_ref, z_own, c_ref, other_ref)
            dot_full(rest_other, z_other, d_ref, left_ref)
            return carry

        lax.fori_loop(0, REFINEMENTS, refine, 0)
        outputs(z_own[...], z_other[...])

    @pl.when(jnp.logical_not(hard))
    def _():
        own = (own_ref[...],)
        y = split(y_ref[...])
        left = other_ref[...].astype(F32) - dot_split(own, y)
        z_other = dot_split(split(left), split(x_ref[...]))
        z_own = dot_split(own, split(first_ref[...])) - dot_split(split(z_other), y, ((1,), (1,)))
        outputs(z_own, z_other)


SMEM = pl.BlockSpec(memory_space=pltpu.SMEM)
VMEM = pl.BlockSpec(memory_space=pltpu.VMEM)


def call(kernel, out_shape, in_specs, mebibytes, megaflops=0, out_specs=VMEM, scratch=()):
    return pl.pallas_call(
        kernel,
        out_shape=out_shape,
        in_specs=in_specs,
        out_specs=out_specs,
        scratch_shapes=scratch,
        compiler_params=pltpu.CompilerParams(vmem_limit_bytes=mebibytes * 2**20),
        cost_estimate=pl.CostEstimate(
            flops=megaflops * 10**6, bytes_accessed=2**20, transcendentals=0
        ),
    )


def exchanged(array, axis):
    devices = lax.axis_size(axis)
    parts = lax.all_to_all(array.reshape(devices, 1, -1), axis, 0, 0, tiled=True)
    return parts.reshape(array.shape)


def from_others(array, axis):
    devices = lax.axis_size(axis)
    return [
        lax.ppermute(array, axis, [(i, (i + shift) % devices) for i in range(devices)])
        for shift in range(1, devices)
    ]


def on_device(grads, labeled, damping):
    _, row_count, width = grads.shape
    count = row_count * lax.axis_size(EX)
    core = lax.axis_index("layer").astype(jnp.int32).reshape(1)
    side = lax.axis_index(PAIR).astype(jnp.int32).reshape(1)
    swap = [(0, 1), (1, 0)]
    own = grads[0]
    labeled = labeled.reshape(1, row_count)
    pair = lax.ppermute(own, PAIR, swap)
    labeled_pair = lax.ppermute(labeled, PAIR, swap)
    other = lax.ppermute(own, "layer", swap)
    damping_other = lax.ppermute(damping, "layer", swap)
    blocks = width // LANES
    rows = blocks * (blocks * LANES + HALF)
    planes = lax.axis_size(FAR)
    square = pltpu.VMEM((width, width), F32)
    matrix = jax.ShapeDtypeStruct((width, width), F32)
    turned = jax.ShapeDtypeStruct((width, row_count), BF16)

    def slabs(length):
        return jax.ShapeDtypeStruct((length, LANES), F32)

    own_t, other_t = call(mask_kernel, (turned, turned), [VMEM] * 3, 8, 2000, (VMEM, VMEM))(
        labeled, own, other
    )
    pair, own_t, other_t = lax.optimization_barrier((pair, own_t, other_t))
    pair_other = lax.ppermute(pair, "layer", swap)
    products = call(
        gram_kernel,
        slabs(rows // 2),
        [SMEM] * 2 + [VMEM] * 5,
        16,
        500,
        scratch=[pltpu.VMEM((2 * width, 2 * row_count), BF16)],
    )(
        jnp.concatenate([core, side]), damping_other, labeled_pair, own_t, other_t, pair, pair_other
    )
    sheet = exchanged(products, SHEET)
    partial = call(sum_kernel, slabs(rows // lax.axis_size(NEAR)), [VMEM], 8, 50)(sheet)
    partials = [partial, *from_others(partial, FAR)]
    total = call(total_kernel, slabs(rows), [VMEM] * planes, 8, 50)(*partials)
    mine = exchanged(total, NEAR)
    theirs = lax.ppermute(mine, "layer", swap)
    first, hard = call(
        functools.partial(first_kernel, count),
        (matrix, jax.ShapeDtypeStruct((1,), jnp.int32)),
        [SMEM, VMEM],
        16,
        3000,
        (VMEM, SMEM),
        [square] * 4,
    )(damping, mine)
    solved, score = call(
        functools.partial(solve_kernel, count),
        (
            jax.ShapeDtypeStruct((row_count, width), F32),
            jax.ShapeDtypeStruct((1, row_count), F32),
        ),
        [SMEM] * 4 + [VMEM] * 5,
        32,
        6000,
        (VMEM, VMEM),
        [square] * 9 + [pltpu.VMEM((row_count, width), F32)],
    )(core, hard, damping, damping_other, mine, theirs, first, own, other)
    return solved[None], score.reshape(row_count)


def solution(mesh):
    torus = Mesh(mesh.devices.reshape(mesh.shape["layer"], 4, 2, 4, 4), ("layer", *EX))
    in_specs = (P("layer", EX, None), P(EX), P("layer"))
    out_specs = (P("layer", EX, None), P(EX))
    return jax.shard_map(
        on_device, mesh=torus, in_specs=in_specs, out_specs=out_specs, check_vma=False
    )
```

```python
import functools

import jax
import jax.numpy as jnp
from jax import lax
from jax.experimental import pallas as pl
from jax.experimental.pallas import tpu as pltpu
from jax.sharding import Mesh
from jax.sharding import PartitionSpec as P

EX = ("z_hi", "z_lo", "y", "x")
FAR, NEAR = EX[0], EX[1:]
F32, BF16 = jnp.float32, jnp.bfloat16
LANES = 128
HALF = LANES // 2
RESIDUAL = 0.002
STEPS = 60
TILES = 4
REFINEMENTS = 3


def dot(a, b, dims=((1,), (0,)), precision=None):
    return lax.dot_general(a, b, (dims, ((), ())), preferred_element_type=F32, precision=precision)


def split(a):
    high = a.astype(BF16)
    return high, (a - high.astype(F32)).astype(BF16)


def dot_split(a, b, dims=((1,), (0,))):
    total = dot(a[0], b[0], dims)
    if len(b) > 1:
        total = total + dot(a[0], b[1], dims)
    if len(a) > 1:
        total = total + dot(a[1], b[0], dims)
    return total


def dot_full(out_ref, a_ref, b, base_ref=None, dims=((1,), (0,))):
    tile = a_ref.shape[0] // TILES

    def step(t, _):
        at = pl.ds(pl.multiple_of(t * tile, tile), tile)
        product = dot(a_ref[at, :].astype(F32), b[...], dims, lax.Precision.HIGHEST)
        out_ref[at, :] = product if base_ref is None else base_ref[at, :].astype(F32) - product
        return 0

    lax.fori_loop(0, TILES, step, 0)


def mask_kernel(
    damp_ref, damp_other_ref, labeled_hbm, own_hbm, own_t_ref, own_ref, keep_ref, damps_ref, labeled_ref, sems
):
    arriving = [
        pltpu.make_async_copy(own_hbm, own_ref, sems.at[0]),
        pltpu.make_async_copy(labeled_hbm, labeled_ref, sems.at[1]),
    ]
    for copy in arriving:
        copy.start()
    damps_ref[:8] = jnp.full((8, LANES), damp_ref[0])
    damps_ref[8:] = jnp.full((8, LANES), damp_other_ref[0])
    for copy in arriving:
        copy.wait()
    keep = (labeled_ref[...] > 0).astype(F32)
    own_t_ref[...] = (own_ref[...].astype(F32).T * keep).astype(BF16)
    keep_ref[...] = keep


def gram_kernel(core_ref, keep_ref, own_t_ref, own_ref, other_ref, out_ref):
    core = core_ref[0]
    keep = keep_ref[...]
    own_t, own, other = own_t_ref[...], own_ref[...], other_ref[...]
    blocks = own.shape[1] // LANES
    first_t = jnp.where(core == 0, own_t, (other.astype(F32).T * keep).astype(BF16))
    last = jnp.where(core == 0, other, own)
    both = jnp.concatenate([own, other], axis=1)
    slab = blocks * LANES + HALF
    for i in range(blocks):
        rows = own_t[i * LANES : (i + 1) * LANES]
        product = dot(rows, both[:, i * LANES : (i + blocks) * LANES])
        for b in range(blocks):
            start = i * slab + b * LANES
            out_ref[start : start + LANES] = product[:, b * LANES : (b + 1) * LANES]
        middle = dot(first_t[i * LANES : (i + 1) * LANES], last[:, i * LANES : (i + 1) * LANES])
        start = i * slab + blocks * LANES
        out_ref[start : start + HALF] = jnp.where(core == 0, middle[:HALF], middle[HALF:])


def sum_kernel(in_ref, out_ref):
    rows = out_ref.shape[0]
    total = in_ref[:rows]
    for part in range(1, in_ref.shape[0] // rows):
        total = total + in_ref[part * rows : (part + 1) * rows]
    out_ref[...] = total


def total_kernel(*refs):
    out_ref = refs[-1]
    total = refs[0][...]
    for ref in refs[1:-1]:
        total = total + ref[...]
    rows = total.shape[0]
    for copy in range(out_ref.shape[0] // rows):
        out_ref[copy * rows : (copy + 1) * rows] = total


def eye(width):
    rows = lax.broadcasted_iota(jnp.int32, (width, width), 0)
    return rows == lax.broadcasted_iota(jnp.int32, (width, width), 1)


def invert(s_ref, a_ref, x_ref, r_ref, t_ref, refresh=None, known_hard=None):
    width = s_ref.shape[0]

    def scales():
        diagonal = jnp.where(eye(width), s_ref[...], 0.0)
        row = lax.rsqrt(jnp.sum(diagonal, axis=0, keepdims=True))
        return lax.rsqrt(jnp.sum(diagonal, axis=1, keepdims=True)), row

    def scaled():
        column, row = scales()
        a_ref[...] = s_ref[...] * column * row

    def square():
        r = r_ref[...].astype(BF16)
        t = dot(r, r)
        t_ref[...] = t
        return jnp.sum(t * t)

    def residual():
        dot_full(r_ref, a_ref, x_ref)
        r_ref[...] = eye(width).astype(F32) - r_ref[...]

    scaled()
    one = eye(width).astype(F32)
    e = one - a_ref[...]
    e1 = e.astype(BF16)
    e2 = dot(e1, e1).astype(BF16)
    x = one + e
    x = (x + dot(x.astype(BF16), e2)).astype(BF16)
    x_ref[...] = x.astype(F32)
    r_ref[...] = one - dot_split(split(a_ref[...]), (x,))
    norm = square()
    hard = jnp.logical_not(norm <= RESIDUAL**2)
    if known_hard is not None:
        hard = jnp.logical_or(hard, known_hard)

    @pl.when(hard)
    def _():
        if refresh is not None:
            refresh()
        scaled()

        @pl.when(jnp.logical_not(norm < 0.25))
        def _():
            largest = jnp.max(jnp.sum(jnp.abs(a_ref[...]), axis=1, keepdims=True))
            x_ref[...] = jnp.where(eye(width), 1.0 / largest, 0.0)

        residual()

        def far(state):
            return jnp.logical_and(state[0] < STEPS, state[1] > 0.01 * RESIDUAL**2)

        def newton(state):
            dot_full(t_ref, x_ref, r_ref)
            x_ref[...] += t_ref[...]
            residual()
            return state[0] + 1, square()

        lax.while_loop(far, newton, (jnp.int32(0), square()))

    step = (r_ref[...] + t_ref[...]).astype(BF16)
    column, row = scales()
    x_ref[...] = (x_ref[...] + dot(x_ref[...].astype(BF16), step)) * column * row
    return hard


def part(ref, i, start, rows, blocks, count):
    at = i * (blocks * LANES + HALF) + start
    return ref[at : at + rows] * (1.0 / count)


def put(ref, i, j, block):
    ref[i * LANES : (i + 1) * LANES, j * LANES : (j + 1) * LANES] = block


def put_diagonal(ref, slabs_ref, damp, count):
    blocks = ref.shape[0] // LANES
    unit = eye(LANES)
    for i in range(blocks):
        put(ref, i, i, part(slabs_ref, i, 0, LANES, blocks, count) + jnp.where(unit, damp, 0.0))
        for j in range(i + 1, blocks):
            block = part(slabs_ref, i, (j - i) * LANES, LANES, blocks, count)
            put(ref, i, j, block)
            put(ref, j, i, block.T)


def first_kernel(count, damp_ref, mine_ref, x_ref, hard_ref, s_ref, a_ref, r_ref, t_ref):
    put_diagonal(s_ref, mine_ref, damp_ref[:1], count)
    hard_ref[0] = invert(s_ref, a_ref, x_ref, r_ref, t_ref).astype(jnp.int32)


def solve_kernel(
    count, core_ref, hard_ref, damps_ref, mine_ref, theirs_ref, first_ref, own_ref, other_ref,
    solved_ref, score_ref, s_ref, d_ref, c_ref, ct_ref, a_ref, x_ref, r_ref, t_ref, y_ref,
    left_ref, z_ref, sems,
):
    near = core_ref[0] == 0
    width = own_ref.shape[1]
    blocks = width // LANES
    damp, damp_other = damps_ref[:1], damps_ref[8:9]

    for i in range(blocks):
        for j in range(i):
            start = (j + blocks - i) * LANES
            block = part(mine_ref, i, start, LANES, blocks, count)
            put(c_ref, i, j, block)
            put(ct_ref, j, i, block.T)
            block = part(theirs_ref, i, start, LANES, blocks, count)
            put(ct_ref, i, j, block)
            put(c_ref, j, i, block.T)
        mine = part(mine_ref, i, blocks * LANES, HALF, blocks, count)
        theirs = part(theirs_ref, i, blocks * LANES, HALF, blocks, count)
        block = jnp.concatenate([jnp.where(near, mine, theirs), jnp.where(near, theirs, mine)], 0)
        turned = block.T
        put(c_ref, i, i, jnp.where(near, block, turned))
        put(ct_ref, i, i, jnp.where(near, turned, block))
    put_diagonal(d_ref, theirs_ref, damp_other, count)

    first = split(first_ref[...])
    y_ref[...] = dot_split(first, split(c_ref[...]))
    s_ref[...] = d_ref[...] - dot_split(split(ct_ref[...]), split(y_ref[...]))

    def refresh():
        dot_full(y_ref, first_ref, c_ref)
        dot_full(s_ref, ct_ref, y_ref, d_ref)

    hard = invert(s_ref, a_ref, x_ref, r_ref, t_ref, refresh, hard_ref[0] > 0)

    half = z_ref.shape[0] // 2
    parts = [pl.ds(0, half), pl.ds(half, half)]
    leaving = [
        pltpu.make_async_copy(z_ref.at[p], solved_ref.at[p], sems.at[i]) for i, p in enumerate(parts)
    ]

    def candidate_sum(terms):
        folded = terms[:, :LANES]
        for b in range(1, blocks):
            folded = folded + terms[:, b * LANES : (b + 1) * LANES]
        return jnp.sum(folded.T, axis=0, keepdims=True)

    def scores(p, z_own, z_other):
        gain = own_ref[p, :].astype(F32) * z_own + other_ref[p, :].astype(F32) * z_other
        gain = candidate_sum(gain)
        penalty = damp * candidate_sum(z_own * z_own) + damp_other * candidate_sum(z_other * z_other)
        return (gain - penalty) / (1.0 + gain)

    def outputs(solve_rows):
        found = []
        for p, copy in zip(parts, leaving):
            z_own, z_other = solve_rows(p)
            z_ref[p, :] = z_own
            copy.start()
            found.append((p, z_own, z_other))
        score_ref[...] = jnp.concatenate([scores(*each) for each in found], axis=1)
        for copy in leaving:
            copy.wait()

    @pl.when(hard)
    def _():
        count_rows = left_ref.shape[0]
        top, bottom = pl.ds(0, count_rows), pl.ds(count_rows, count_rows)
        z_own, z_other = a_ref.at[top], a_ref.at[bottom]
        rest_own, rest_other = r_ref.at[top], r_ref.at[bottom]
        step_own, step_other = t_ref.at[top], t_ref.at[bottom]
        put_diagonal(s_ref, mine_ref, damp, count)
        a_ref[...] = jnp.zeros_like(a_ref)
        rest_own[...] = own_ref[...].astype(F32)
        rest_other[...] = other_ref[...].astype(F32)

        def refine(_, carry):
            dot_full(left_ref, rest_own, y_ref, rest_other)
            dot_full(step_other, left_ref, x_ref)
            dot_full(left_ref, rest_own, first_ref)
            dot_full(step_own, step_other, y_ref, left_ref, ((1,), (1,)))
            a_ref[...] += t_ref[...]
            dot_full(left_ref, z_own, s_ref, own_ref)
            dot_full(rest_own, z_other, ct_ref, left_ref)
            dot_full(left_ref, z_own, c_ref, other_ref)
            dot_full(rest_other, z_other, d_ref, left_ref)
            return carry

        lax.fori_loop(0, REFINEMENTS, refine, 0)
        outputs(lambda p: (z_own[p, :], z_other[p, :]))

    @pl.when(jnp.logical_not(hard))
    def _():
        y, x, p0 = split(y_ref[...]), split(x_ref[...]), split(first_ref[...])

        def solve_rows(p):
            own = (own_ref[p, :],)
            left = other_ref[p, :].astype(F32) - dot_split(own, y)
            z_other = dot_split(split(left), x)
            return dot_split(own, p0) - dot_split(split(z_other), y, ((1,), (1,))), z_other

        outputs(solve_rows)


SMEM = pl.BlockSpec(memory_space=pltpu.SMEM)
VMEM = pl.BlockSpec(memory_space=pltpu.VMEM)
HBM = pl.BlockSpec(memory_space=pltpu.HBM)


def call(kernel, out_shape, in_specs, mebibytes, megaflops=0, out_specs=VMEM, scratch=()):
    return pl.pallas_call(
        kernel,
        out_shape=out_shape,
        in_specs=in_specs,
        out_specs=out_specs,
        scratch_shapes=scratch,
        compiler_params=pltpu.CompilerParams(vmem_limit_bytes=mebibytes * 2**20),
        cost_estimate=pl.CostEstimate(
            flops=megaflops * 10**6, bytes_accessed=2**20, transcendentals=0
        ),
    )


def exchanged(array, axis):
    devices = lax.axis_size(axis)
    parts = lax.all_to_all(array.reshape(devices, 1, -1), axis, 0, 0, tiled=True)
    return parts.reshape(array.shape)


def from_others(array, axis):
    devices = lax.axis_size(axis)
    return [
        lax.ppermute(array, axis, [(i, (i + shift) % devices) for i in range(devices)])
        for shift in range(1, devices)
    ]


def on_device(grads, labeled, damping):
    _, row_count, width = grads.shape
    count = row_count * lax.axis_size(EX)
    core = lax.axis_index("layer").astype(jnp.int32).reshape(1)
    swap = [(0, 1), (1, 0)]
    own = grads[0]
    labeled = labeled.reshape(1, row_count)
    other = lax.ppermute(own, "layer", swap)
    damping_other = lax.ppermute(damping, "layer", swap)
    blocks = width // LANES
    rows = blocks * (blocks * LANES + HALF)
    pieces, planes = lax.axis_size(NEAR), lax.axis_size(FAR)
    square = pltpu.VMEM((width, width), F32)
    matrix = jax.ShapeDtypeStruct((width, width), F32)

    def slabs(length):
        return jax.ShapeDtypeStruct((length, LANES), F32)

    own_t, own, keep, damps = call(
        mask_kernel,
        (
            jax.ShapeDtypeStruct((width, row_count), BF16),
            jax.ShapeDtypeStruct((row_count, width), BF16),
            jax.ShapeDtypeStruct((1, row_count), F32),
            jax.ShapeDtypeStruct((16, LANES), F32),
        ),
        [SMEM, SMEM, HBM, HBM],
        8,
        2000,
        (VMEM,) * 4,
        [pltpu.VMEM((1, row_count), jnp.int32), pltpu.SemaphoreType.DMA((2,))],
    )(damping, damping_other, labeled, own)
    products = call(gram_kernel, slabs(rows), [SMEM] + [VMEM] * 4, 16, 500)(
        core, keep, own_t, own, other
    )
    partial = call(sum_kernel, slabs(rows // pieces), [VMEM], 8, 50)(exchanged(products, NEAR))
    partials = [partial, *from_others(partial, FAR)]
    total = call(total_kernel, slabs(rows), [VMEM] * planes, 8, 50)(*partials)
    mine = exchanged(total, NEAR)
    theirs = lax.ppermute(mine, "layer", swap)
    first, hard = call(
        functools.partial(first_kernel, count),
        (matrix, jax.ShapeDtypeStruct((1,), jnp.int32)),
        [VMEM] * 2,
        16,
        3000,
        (VMEM, SMEM),
        [square] * 4,
    )(damps, mine)
    solved, score = call(
        functools.partial(solve_kernel, count),
        (
            jax.ShapeDtypeStruct((row_count, width), F32),
            jax.ShapeDtypeStruct((1, row_count), F32),
        ),
        [SMEM] * 2 + [VMEM] * 6,
        32,
        6000,
        (pl.BlockSpec(memory_space=pl.ANY), VMEM),
        [square] * 9 + [pltpu.VMEM((row_count, width), F32)] * 2 + [pltpu.SemaphoreType.DMA((2,))],
    )(core, hard, damps, mine, theirs, first, own, other)
    return solved[None], score.reshape(row_count)


def solution(mesh):
    torus = Mesh(mesh.devices.reshape(mesh.shape["layer"], 4, 2, 4, 4), ("layer", *EX))
    in_specs = (P("layer", EX, None), P(EX), P("layer"))
    out_specs = (P("layer", EX, None), P(EX))
    return jax.shard_map(
        on_device, mesh=torus, in_specs=in_specs, out_specs=out_specs, check_vma=False
    )
```

```python
import functools

import jax
import jax.numpy as jnp
from jax import lax
from jax.experimental import pallas as pl
from jax.experimental.pallas import tpu as pltpu
from jax.sharding import Mesh
from jax.sharding import PartitionSpec as P

EX = ("z_hi", "z_lo", "y", "x")
FAR, NEAR = EX[0], EX[1:]
F32, BF16 = jnp.float32, jnp.bfloat16
LANES = 128
HALF = LANES // 2
RESIDUAL = 0.002
STEPS = 60
TILES = 4
REFINEMENTS = 3


def dot(a, b, dims=((1,), (0,)), precision=None):
    return lax.dot_general(a, b, (dims, ((), ())), preferred_element_type=F32, precision=precision)


def split(a):
    high = a.astype(BF16)
    return high, (a - high.astype(F32)).astype(BF16)


def dot_split(a, b, dims=((1,), (0,))):
    total = dot(a[0], b[0], dims)
    if len(b) > 1:
        total = total + dot(a[0], b[1], dims)
    if len(a) > 1:
        total = total + dot(a[1], b[0], dims)
    return total


def dot_full(out_ref, a_ref, b, base_ref=None, dims=((1,), (0,))):
    tile = a_ref.shape[0] // TILES

    def step(t, _):
        at = pl.ds(pl.multiple_of(t * tile, tile), tile)
        product = dot(a_ref[at, :].astype(F32), b[...], dims, lax.Precision.HIGHEST)
        out_ref[at, :] = product if base_ref is None else base_ref[at, :].astype(F32) - product
        return 0

    lax.fori_loop(0, TILES, step, 0)


def mask_kernel(labeled_ref, own_ref, own_t_ref, rows_ref, keep_ref):
    keep = (labeled_ref[...] > 0).astype(F32)
    own_t_ref[...] = (own_ref[...].astype(F32).T * keep).astype(BF16)
    rows_ref[...] = own_ref[...]
    keep_ref[...] = keep


def gram_kernel(
    core_ref, damp_ref, damp_other_ref, keep_ref, own_t_ref, own_ref, other_ref, out_ref, damps_ref
):
    damps_ref[:8] = jnp.full((8, LANES), damp_ref[0])
    damps_ref[8:] = jnp.full((8, LANES), damp_other_ref[0])
    core = core_ref[0]
    keep = keep_ref[...]
    own_t, own, other = own_t_ref[...], own_ref[...], other_ref[...]
    blocks = own.shape[1] // LANES
    first_t = jnp.where(core == 0, own_t, (other.astype(F32).T * keep).astype(BF16))
    last = jnp.where(core == 0, other, own)
    both = jnp.concatenate([own, other], axis=1)
    slab = blocks * LANES + HALF
    for i in range(blocks):
        rows = own_t[i * LANES : (i + 1) * LANES]
        product = dot(rows, both[:, i * LANES : (i + blocks) * LANES])
        for b in range(blocks):
            start = i * slab + b * LANES
            out_ref[start : start + LANES] = product[:, b * LANES : (b + 1) * LANES]
        middle = dot(first_t[i * LANES : (i + 1) * LANES], last[:, i * LANES : (i + 1) * LANES])
        start = i * slab + blocks * LANES
        out_ref[start : start + HALF] = jnp.where(core == 0, middle[:HALF], middle[HALF:])


def sum_kernel(in_ref, out_ref):
    rows = out_ref.shape[0]
    total = in_ref[:rows]
    for part in range(1, in_ref.shape[0] // rows):
        total = total + in_ref[part * rows : (part + 1) * rows]
    out_ref[...] = total


def total_kernel(*refs):
    out_ref = refs[-1]
    total = refs[0][...]
    for ref in refs[1:-1]:
        total = total + ref[...]
    rows = total.shape[0]
    for copy in range(out_ref.shape[0] // rows):
        out_ref[copy * rows : (copy + 1) * rows] = total


def eye(width):
    rows = lax.broadcasted_iota(jnp.int32, (width, width), 0)
    return rows == lax.broadcasted_iota(jnp.int32, (width, width), 1)


def invert(s_ref, a_ref, x_ref, r_ref, t_ref, refresh=None, known_hard=None):
    width = s_ref.shape[0]

    def scales():
        diagonal = jnp.where(eye(width), s_ref[...], 0.0)
        row = lax.rsqrt(jnp.sum(diagonal, axis=0, keepdims=True))
        return lax.rsqrt(jnp.sum(diagonal, axis=1, keepdims=True)), row

    def scaled():
        column, row = scales()
        a_ref[...] = s_ref[...] * column * row

    def square():
        r = r_ref[...].astype(BF16)
        t = dot(r, r)
        t_ref[...] = t
        return jnp.sum(t * t)

    def residual():
        dot_full(r_ref, a_ref, x_ref)
        r_ref[...] = eye(width).astype(F32) - r_ref[...]

    scaled()
    one = eye(width).astype(F32)
    e = one - a_ref[...]
    e1 = e.astype(BF16)
    e2 = dot(e1, e1).astype(BF16)
    x = one + e
    x = (x + dot(x.astype(BF16), e2)).astype(BF16)
    x_ref[...] = x.astype(F32)
    r_ref[...] = one - dot_split(split(a_ref[...]), (x,))
    norm = square()
    hard = jnp.logical_not(norm <= RESIDUAL**2)
    if known_hard is not None:
        hard = jnp.logical_or(hard, known_hard)

    @pl.when(hard)
    def _():
        if refresh is not None:
            refresh()
        scaled()

        @pl.when(jnp.logical_not(norm < 0.25))
        def _():
            largest = jnp.max(jnp.sum(jnp.abs(a_ref[...]), axis=1, keepdims=True))
            x_ref[...] = jnp.where(eye(width), 1.0 / largest, 0.0)

        residual()

        def far(state):
            return jnp.logical_and(state[0] < STEPS, state[1] > 0.01 * RESIDUAL**2)

        def newton(state):
            dot_full(t_ref, x_ref, r_ref)
            x_ref[...] += t_ref[...]
            residual()
            return state[0] + 1, square()

        lax.while_loop(far, newton, (jnp.int32(0), square()))

    step = (r_ref[...] + t_ref[...]).astype(BF16)
    column, row = scales()
    x_ref[...] = (x_ref[...] + dot(x_ref[...].astype(BF16), step)) * column * row
    return hard


def part(ref, i, start, rows, blocks, count):
    at = i * (blocks * LANES + HALF) + start
    return ref[at : at + rows] * (1.0 / count)


def put(ref, i, j, block):
    ref[i * LANES : (i + 1) * LANES, j * LANES : (j + 1) * LANES] = block


def put_diagonal(ref, slabs_ref, damp, count):
    blocks = ref.shape[0] // LANES
    unit = eye(LANES)
    for i in range(blocks):
        put(ref, i, i, part(slabs_ref, i, 0, LANES, blocks, count) + jnp.where(unit, damp, 0.0))
        for j in range(i + 1, blocks):
            block = part(slabs_ref, i, (j - i) * LANES, LANES, blocks, count)
            put(ref, i, j, block)
            put(ref, j, i, block.T)


def first_kernel(count, damp_ref, mine_ref, x_ref, hard_ref, s_ref, a_ref, r_ref, t_ref):
    put_diagonal(s_ref, mine_ref, damp_ref[:1], count)
    hard_ref[0] = invert(s_ref, a_ref, x_ref, r_ref, t_ref).astype(jnp.int32)


def solve_kernel(
    count, core_ref, hard_ref, damps_ref, mine_ref, theirs_ref, first_ref, own_ref, other_ref,
    solved_ref, score_ref, s_ref, d_ref, c_ref, ct_ref, a_ref, x_ref, r_ref, t_ref, y_ref,
    left_ref, z_ref, sem,
):
    near = core_ref[0] == 0
    width = own_ref.shape[1]
    blocks = width // LANES
    damp, damp_other = damps_ref[:1], damps_ref[8:9]

    for i in range(blocks):
        for j in range(i):
            start = (j + blocks - i) * LANES
            block = part(mine_ref, i, start, LANES, blocks, count)
            put(c_ref, i, j, block)
            put(ct_ref, j, i, block.T)
            block = part(theirs_ref, i, start, LANES, blocks, count)
            put(ct_ref, i, j, block)
            put(c_ref, j, i, block.T)
        mine = part(mine_ref, i, blocks * LANES, HALF, blocks, count)
        theirs = part(theirs_ref, i, blocks * LANES, HALF, blocks, count)
        block = jnp.concatenate([jnp.where(near, mine, theirs), jnp.where(near, theirs, mine)], 0)
        turned = block.T
        put(c_ref, i, i, jnp.where(near, block, turned))
        put(ct_ref, i, i, jnp.where(near, turned, block))
    put_diagonal(d_ref, theirs_ref, damp_other, count)

    first = split(first_ref[...])
    y_ref[...] = dot_split(first, split(c_ref[...]))
    s_ref[...] = d_ref[...] - dot_split(split(ct_ref[...]), split(y_ref[...]))

    def refresh():
        dot_full(y_ref, first_ref, c_ref)
        dot_full(s_ref, ct_ref, y_ref, d_ref)

    hard = invert(s_ref, a_ref, x_ref, r_ref, t_ref, refresh, hard_ref[0] > 0)

    leaving = pltpu.make_async_copy(z_ref, solved_ref, sem)

    def candidate_sum(terms):
        folded = terms[:, :LANES]
        for b in range(1, blocks):
            folded = folded + terms[:, b * LANES : (b + 1) * LANES]
        return jnp.sum(folded.T, axis=0, keepdims=True)

    def outputs(z_own, z_other):
        z_ref[...] = z_own
        leaving.start()
        gain = candidate_sum(own_ref[...].astype(F32) * z_own + other_ref[...].astype(F32) * z_other)
        wide = (z_own.shape[0] // LANES,)
        penalty = jnp.tile(damp, wide) * candidate_sum(z_own * z_own)
        penalty = penalty + jnp.tile(damp_other, wide) * candidate_sum(z_other * z_other)
        score_ref[...] = (gain - penalty) / (1.0 + gain)
        leaving.wait()

    @pl.when(hard)
    def _():
        count_rows = left_ref.shape[0]
        top, bottom = pl.ds(0, count_rows), pl.ds(count_rows, count_rows)
        z_own, z_other = a_ref.at[top], a_ref.at[bottom]
        rest_own, rest_other = r_ref.at[top], r_ref.at[bottom]
        step_own, step_other = t_ref.at[top], t_ref.at[bottom]
        put_diagonal(s_ref, mine_ref, damp, count)
        a_ref[...] = jnp.zeros_like(a_ref)
        rest_own[...] = own_ref[...].astype(F32)
        rest_other[...] = other_ref[...].astype(F32)

        def refine(_, carry):
            dot_full(left_ref, rest_own, y_ref, rest_other)
            dot_full(step_other, left_ref, x_ref)
            dot_full(left_ref, rest_own, first_ref)
            dot_full(step_own, step_other, y_ref, left_ref, ((1,), (1,)))
            a_ref[...] += t_ref[...]
            dot_full(left_ref, z_own, s_ref, own_ref)
            dot_full(rest_own, z_other, ct_ref, left_ref)
            dot_full(left_ref, z_own, c_ref, other_ref)
            dot_full(rest_other, z_other, d_ref, left_ref)
            return carry

        lax.fori_loop(0, REFINEMENTS, refine, 0)
        outputs(z_own[...], z_other[...])

    @pl.when(jnp.logical_not(hard))
    def _():
        own, y = (own_ref[...],), split(y_ref[...])
        left = other_ref[...].astype(F32) - dot_split(own, y)
        z_other = dot_split(split(left), split(x_ref[...]))
        z_own = dot_split(own, split(first_ref[...])) - dot_split(split(z_other), y, ((1,), (1,)))
        outputs(z_own, z_other)


SMEM = pl.BlockSpec(memory_space=pltpu.SMEM)
VMEM = pl.BlockSpec(memory_space=pltpu.VMEM)


def call(kernel, out_shape, in_specs, mebibytes, megaflops=0, out_specs=VMEM, scratch=()):
    return pl.pallas_call(
        kernel,
        out_shape=out_shape,
        in_specs=in_specs,
        out_specs=out_specs,
        scratch_shapes=scratch,
        compiler_params=pltpu.CompilerParams(vmem_limit_bytes=mebibytes * 2**20),
        cost_estimate=pl.CostEstimate(
            flops=megaflops * 10**6, bytes_accessed=2**20, transcendentals=0
        ),
    )


def exchanged(array, axis):
    devices = lax.axis_size(axis)
    parts = lax.all_to_all(array.reshape(devices, 1, -1), axis, 0, 0, tiled=True)
    return parts.reshape(array.shape)


def from_others(array, axis):
    devices = lax.axis_size(axis)
    return [
        lax.ppermute(array, axis, [(i, (i + shift) % devices) for i in range(devices)])
        for shift in range(1, devices)
    ]


def on_device(grads, labeled, damping):
    _, row_count, width = grads.shape
    count = row_count * lax.axis_size(EX)
    core = lax.axis_index("layer").astype(jnp.int32).reshape(1)
    swap = [(0, 1), (1, 0)]
    own = grads[0]
    labeled = labeled.reshape(1, row_count)
    other = lax.ppermute(own, "layer", swap)
    damping_other = lax.ppermute(damping, "layer", swap)
    blocks = width // LANES
    rows = blocks * (blocks * LANES + HALF)
    pieces, planes = lax.axis_size(NEAR), lax.axis_size(FAR)
    square = pltpu.VMEM((width, width), F32)
    matrix = jax.ShapeDtypeStruct((width, width), F32)

    def slabs(length):
        return jax.ShapeDtypeStruct((length, LANES), F32)

    own_t, own, keep = call(
        mask_kernel,
        (
            jax.ShapeDtypeStruct((width, row_count), BF16),
            jax.ShapeDtypeStruct((row_count, width), BF16),
            jax.ShapeDtypeStruct((1, row_count), F32),
        ),
        [VMEM] * 2,
        8,
        2000,
        (VMEM,) * 3,
    )(labeled, own)
    products, damps = call(
        gram_kernel,
        (slabs(rows), slabs(16)),
        [SMEM] * 3 + [VMEM] * 4,
        16,
        500,
        (VMEM,) * 2,
    )(core, damping, damping_other, keep, own_t, own, other)
    partial = call(sum_kernel, slabs(rows // pieces), [VMEM], 8, 50)(exchanged(products, NEAR))
    partials = [partial, *from_others(partial, FAR)]
    total = call(total_kernel, slabs(rows), [VMEM] * planes, 8, 50)(*partials)
    mine = exchanged(total, NEAR)
    theirs = lax.ppermute(mine, "layer", swap)
    first, hard = call(
        functools.partial(first_kernel, count),
        (matrix, jax.ShapeDtypeStruct((1,), jnp.int32)),
        [VMEM] * 2,
        16,
        3000,
        (VMEM, SMEM),
        [square] * 4,
    )(damps, mine)
    solved, score = call(
        functools.partial(solve_kernel, count),
        (
            jax.ShapeDtypeStruct((row_count, width), F32),
            jax.ShapeDtypeStruct((1, row_count), F32),
        ),
        [SMEM] * 2 + [VMEM] * 6,
        32,
        6000,
        (pl.BlockSpec(memory_space=pl.ANY), VMEM),
        [square] * 9 + [pltpu.VMEM((row_count, width), F32)] * 2 + [pltpu.SemaphoreType.DMA],
    )(core, hard, damps, mine, theirs, first, own, other)
    return solved[None], score.reshape(row_count)


def solution(mesh):
    torus = Mesh(mesh.devices.reshape(mesh.shape["layer"], 4, 2, 4, 4), ("layer", *EX))
    in_specs = (P("layer", EX, None), P(EX), P("layer"))
    out_specs = (P("layer", EX, None), P(EX))
    return jax.shard_map(
        on_device, mesh=torus, in_specs=in_specs, out_specs=out_specs, check_vma=False
    )
```

```python
import functools

import jax
import jax.numpy as jnp
from jax import lax
from jax.experimental import pallas as pl
from jax.experimental.pallas import tpu as pltpu
from jax.sharding import Mesh
from jax.sharding import PartitionSpec as P

EX = ("z_hi", "z_lo", "y", "x")
FAR, NEAR = EX[0], EX[1:]
F32, BF16 = jnp.float32, jnp.bfloat16
LANES = 128
HALF = LANES // 2
DIAGONAL = HALF + HALF // 2
RESIDUAL = 0.002
STEPS = 60
TILES = 4
REFINEMENTS = 3


def slab_rows(blocks):
    return DIAGONAL + (blocks - 1) * LANES + HALF


def dot(a, b, dims=((1,), (0,)), precision=None):
    return lax.dot_general(a, b, (dims, ((), ())), preferred_element_type=F32, precision=precision)


def split(a):
    high = a.astype(BF16)
    return high, (a - high.astype(F32)).astype(BF16)


def dot_split(a, b, dims=((1,), (0,))):
    total = dot(a[0], b[0], dims)
    if len(b) > 1:
        total = total + dot(a[0], b[1], dims)
    if len(a) > 1:
        total = total + dot(a[1], b[0], dims)
    return total


def dot_full(out_ref, a_ref, b, base_ref=None, dims=((1,), (0,))):
    tile = a_ref.shape[0] // TILES

    def step(t, _):
        at = pl.ds(pl.multiple_of(t * tile, tile), tile)
        product = dot(a_ref[at, :].astype(F32), b[...], dims, lax.Precision.HIGHEST)
        out_ref[at, :] = product if base_ref is None else base_ref[at, :].astype(F32) - product
        return 0

    lax.fori_loop(0, TILES, step, 0)


def mask_kernel(labeled_hbm, own_hbm, own_t_ref, own_ref, keep_ref, labeled_ref, sems):
    arriving = [
        pltpu.make_async_copy(own_hbm, own_ref, sems.at[0]),
        pltpu.make_async_copy(labeled_hbm, labeled_ref, sems.at[1]),
    ]
    for copy in arriving:
        copy.start()
    for copy in arriving:
        copy.wait()
    keep = (labeled_ref[...] > 0).astype(F32)
    own_t_ref[...] = (own_ref[...].astype(F32).T * keep).astype(BF16)
    keep_ref[...] = keep


def gram_kernel(core_ref, keep_ref, own_t_ref, own_ref, other_ref, out_ref):
    core = core_ref[0]
    keep = keep_ref[...]
    own_t, own, other = own_t_ref[...], own_ref[...], other_ref[...]
    blocks = own.shape[1] // LANES
    first_t = jnp.where(core == 0, own_t, (other.astype(F32).T * keep).astype(BF16))
    last = jnp.where(core == 0, other, own)
    both = jnp.concatenate([own, other], axis=1)
    slab = slab_rows(blocks)
    left = lax.broadcasted_iota(jnp.int32, (HALF // 2, LANES), 1) < HALF
    for i in range(blocks):
        rows = own_t[i * LANES : (i + 1) * LANES]
        product = dot(rows, both[:, i * LANES : (i + blocks) * LANES])
        start = i * slab
        out_ref[start : start + HALF] = product[:HALF, :LANES]
        upper, lower = product[HALF : HALF + HALF // 2, :LANES], product[HALF + HALF // 2 :, :LANES]
        start = i * slab + HALF
        out_ref[start : start + HALF // 2] = jnp.where(left, pltpu.roll(upper, HALF, 1), lower)
        for b in range(1, blocks):
            start = i * slab + DIAGONAL + (b - 1) * LANES
            out_ref[start : start + LANES] = product[:, b * LANES : (b + 1) * LANES]
        middle = dot(first_t[i * LANES : (i + 1) * LANES], last[:, i * LANES : (i + 1) * LANES])
        start = (i + 1) * slab - HALF
        out_ref[start : start + HALF] = jnp.where(core == 0, middle[:HALF], middle[HALF:])


def damp_kernel(damp_ref, damp_other_ref, damps_ref):
    damps_ref[:8] = jnp.full((8, LANES), damp_ref[0])
    damps_ref[8:] = jnp.full((8, LANES), damp_other_ref[0])


def sum_kernel(in_ref, out_ref):
    rows = out_ref.shape[0]
    total = in_ref[:rows]
    for part in range(1, in_ref.shape[0] // rows):
        total = total + in_ref[part * rows : (part + 1) * rows]
    out_ref[...] = total


def total_kernel(*refs):
    out_ref = refs[-1]
    total = refs[0][...]
    for ref in refs[1:-1]:
        total = total + ref[...]
    rows = total.shape[0]
    for copy in range(out_ref.shape[0] // rows):
        out_ref[copy * rows : (copy + 1) * rows] = total


def eye(width):
    rows = lax.broadcasted_iota(jnp.int32, (width, width), 0)
    return rows == lax.broadcasted_iota(jnp.int32, (width, width), 1)


def invert(s_ref, a_ref, x_ref, r_ref, t_ref, refresh=None, known_hard=None):
    width = s_ref.shape[0]

    def scales():
        diagonal = jnp.where(eye(width), s_ref[...], 0.0)
        row = lax.rsqrt(jnp.sum(diagonal, axis=0, keepdims=True))
        return lax.rsqrt(jnp.sum(diagonal, axis=1, keepdims=True)), row

    def scaled():
        column, row = scales()
        a_ref[...] = s_ref[...] * column * row

    def square():
        r = r_ref[...].astype(BF16)
        t = dot(r, r)
        t_ref[...] = t
        return jnp.sum(t * t)

    def residual():
        dot_full(r_ref, a_ref, x_ref)
        r_ref[...] = eye(width).astype(F32) - r_ref[...]

    scaled()
    one = eye(width).astype(F32)
    e = one - a_ref[...]
    e1 = e.astype(BF16)
    e2 = dot(e1, e1).astype(BF16)
    x = one + e
    x = (x + dot(x.astype(BF16), e2)).astype(BF16)
    x_ref[...] = x.astype(F32)
    r_ref[...] = one - dot_split(split(a_ref[...]), (x,))
    norm = square()
    hard = jnp.logical_not(norm <= RESIDUAL**2)
    if known_hard is not None:
        hard = jnp.logical_or(hard, known_hard)

    @pl.when(hard)
    def _():
        if refresh is not None:
            refresh()
        scaled()

        @pl.when(jnp.logical_not(norm < 0.25))
        def _():
            largest = jnp.max(jnp.sum(jnp.abs(a_ref[...]), axis=1, keepdims=True))
            x_ref[...] = jnp.where(eye(width), 1.0 / largest, 0.0)

        residual()

        def far(state):
            return jnp.logical_and(state[0] < STEPS, state[1] > 0.01 * RESIDUAL**2)

        def newton(state):
            dot_full(t_ref, x_ref, r_ref)
            x_ref[...] += t_ref[...]
            residual()
            return state[0] + 1, square()

        lax.while_loop(far, newton, (jnp.int32(0), square()))

    step = (r_ref[...] + t_ref[...]).astype(BF16)
    column, row = scales()
    x_ref[...] = (x_ref[...] + dot(x_ref[...].astype(BF16), step)) * column * row
    return hard


def part(ref, i, start, rows, blocks, count):
    at = i * slab_rows(blocks) + start
    return ref[at : at + rows] * (1.0 / count)


def whole_part(ref, i, b, blocks, count):
    return part(ref, i, DIAGONAL + (b - 1) * LANES, LANES, blocks, count)


def diagonal_part(ref, i, blocks, count):
    upper = part(ref, i, 0, HALF, blocks, count)
    packed = part(ref, i, HALF, HALF // 2, blocks, count)
    corner = jnp.concatenate([pltpu.roll(packed, HALF, 1), packed], axis=0)
    left = lax.broadcasted_iota(jnp.int32, (HALF, LANES), 1) < HALF
    turned = jnp.concatenate([upper, corner], axis=0).T
    return jnp.concatenate([upper, jnp.where(left, turned[HALF:], corner)], axis=0)


def put(ref, i, j, block):
    ref[i * LANES : (i + 1) * LANES, j * LANES : (j + 1) * LANES] = block


def put_diagonal(ref, slabs_ref, damp, count):
    blocks = ref.shape[0] // LANES
    unit = eye(LANES)
    for i in range(blocks):
        put(ref, i, i, diagonal_part(slabs_ref, i, blocks, count) + jnp.where(unit, damp, 0.0))
        for j in range(i + 1, blocks):
            block = whole_part(slabs_ref, i, j - i, blocks, count)
            put(ref, i, j, block)
            put(ref, j, i, block.T)


def first_kernel(count, damp_ref, mine_ref, x_ref, hard_ref, s_ref, a_ref, r_ref, t_ref):
    put_diagonal(s_ref, mine_ref, damp_ref[:1], count)
    hard_ref[0] = invert(s_ref, a_ref, x_ref, r_ref, t_ref).astype(jnp.int32)


def solve_kernel(
    count, core_ref, hard_ref, damps_ref, mine_ref, theirs_ref, first_ref, own_ref, other_ref,
    solved_ref, score_ref, s_ref, d_ref, c_ref, ct_ref, a_ref, x_ref, r_ref, t_ref, y_ref,
    left_ref, z_ref, sem,
):
    near = core_ref[0] == 0
    width = own_ref.shape[1]
    blocks = width // LANES
    damp, damp_other = damps_ref[:1], damps_ref[8:9]

    for i in range(blocks):
        for j in range(i):
            block = whole_part(mine_ref, i, j + blocks - i, blocks, count)
            put(c_ref, i, j, block)
            put(ct_ref, j, i, block.T)
            block = whole_part(theirs_ref, i, j + blocks - i, blocks, count)
            put(ct_ref, i, j, block)
            put(c_ref, j, i, block.T)
        last = slab_rows(blocks) - HALF
        mine = part(mine_ref, i, last, HALF, blocks, count)
        theirs = part(theirs_ref, i, last, HALF, blocks, count)
        block = jnp.concatenate([jnp.where(near, mine, theirs), jnp.where(near, theirs, mine)], 0)
        turned = block.T
        put(c_ref, i, i, jnp.where(near, block, turned))
        put(ct_ref, i, i, jnp.where(near, turned, block))
    put_diagonal(d_ref, theirs_ref, damp_other, count)

    first = split(first_ref[...])
    y_ref[...] = dot_split(first, split(c_ref[...]))
    s_ref[...] = d_ref[...] - dot_split(split(ct_ref[...]), split(y_ref[...]))

    def refresh():
        dot_full(y_ref, first_ref, c_ref)
        dot_full(s_ref, ct_ref, y_ref, d_ref)

    hard = invert(s_ref, a_ref, x_ref, r_ref, t_ref, refresh, hard_ref[0] > 0)

    leaving = pltpu.make_async_copy(z_ref, solved_ref, sem)

    def candidate_sum(terms):
        folded = terms[:, :LANES]
        for b in range(1, blocks):
            folded = folded + terms[:, b * LANES : (b + 1) * LANES]
        return jnp.sum(folded.T, axis=0, keepdims=True)

    def outputs(z_own, z_other):
        z_ref[...] = z_own
        leaving.start()
        gain = candidate_sum(own_ref[...].astype(F32) * z_own + other_ref[...].astype(F32) * z_other)
        wide = (z_own.shape[0] // LANES,)
        penalty = jnp.tile(damp, wide) * candidate_sum(z_own * z_own)
        penalty = penalty + jnp.tile(damp_other, wide) * candidate_sum(z_other * z_other)
        score_ref[...] = (gain - penalty) / (1.0 + gain)
        leaving.wait()

    @pl.when(hard)
    def _():
        count_rows = left_ref.shape[0]
        top, bottom = pl.ds(0, count_rows), pl.ds(count_rows, count_rows)
        z_own, z_other = a_ref.at[top], a_ref.at[bottom]
        rest_own, rest_other = r_ref.at[top], r_ref.at[bottom]
        step_own, step_other = t_ref.at[top], t_ref.at[bottom]
        put_diagonal(s_ref, mine_ref, damp, count)
        a_ref[...] = jnp.zeros_like(a_ref)
        rest_own[...] = own_ref[...].astype(F32)
        rest_other[...] = other_ref[...].astype(F32)

        def refine(_, carry):
            dot_full(left_ref, rest_own, y_ref, rest_other)
            dot_full(step_other, left_ref, x_ref)
            dot_full(left_ref, rest_own, first_ref)
            dot_full(step_own, step_other, y_ref, left_ref, ((1,), (1,)))
            a_ref[...] += t_ref[...]
            dot_full(left_ref, z_own, s_ref, own_ref)
            dot_full(rest_own, z_other, ct_ref, left_ref)
            dot_full(left_ref, z_own, c_ref, other_ref)
            dot_full(rest_other, z_other, d_ref, left_ref)
            return carry

        lax.fori_loop(0, REFINEMENTS, refine, 0)
        outputs(z_own[...], z_other[...])

    @pl.when(jnp.logical_not(hard))
    def _():
        own, y = (own_ref[...],), split(y_ref[...])
        left = other_ref[...].astype(F32) - dot_split(own, y)
        z_other = dot_split(split(left), split(x_ref[...]))
        z_own = dot_split(own, split(first_ref[...])) - dot_split(split(z_other), y, ((1,), (1,)))
        outputs(z_own, z_other)


SMEM = pl.BlockSpec(memory_space=pltpu.SMEM)
VMEM = pl.BlockSpec(memory_space=pltpu.VMEM)


def call(kernel, out_shape, in_specs, mebibytes, megaflops=0, out_specs=VMEM, scratch=()):
    return pl.pallas_call(
        kernel,
        out_shape=out_shape,
        in_specs=in_specs,
        out_specs=out_specs,
        scratch_shapes=scratch,
        compiler_params=pltpu.CompilerParams(vmem_limit_bytes=mebibytes * 2**20),
        cost_estimate=pl.CostEstimate(
            flops=megaflops * 10**6, bytes_accessed=2**20, transcendentals=0
        ),
    )


def exchanged(array, axis):
    devices = lax.axis_size(axis)
    parts = lax.all_to_all(array.reshape(devices, 1, -1), axis, 0, 0, tiled=True)
    return parts.reshape(array.shape)


def from_others(array, axis):
    devices = lax.axis_size(axis)
    return [
        lax.ppermute(array, axis, [(i, (i + shift) % devices) for i in range(devices)])
        for shift in range(1, devices)
    ]


def on_device(grads, labeled, damping):
    _, row_count, width = grads.shape
    count = row_count * lax.axis_size(EX)
    core = lax.axis_index("layer").astype(jnp.int32).reshape(1)
    swap = [(0, 1), (1, 0)]
    own = grads[0]
    labeled = labeled.reshape(1, row_count)
    other = lax.ppermute(own, "layer", swap)
    blocks = width // LANES
    rows = blocks * slab_rows(blocks)
    planes = lax.axis_size(FAR)
    square = pltpu.VMEM((width, width), F32)
    matrix = jax.ShapeDtypeStruct((width, width), F32)

    def slabs(length):
        return jax.ShapeDtypeStruct((length, LANES), F32)

    own_t, own, keep = call(
        mask_kernel,
        (
            jax.ShapeDtypeStruct((width, row_count), BF16),
            jax.ShapeDtypeStruct((row_count, width), BF16),
            jax.ShapeDtypeStruct((1, row_count), F32),
        ),
        [pl.BlockSpec(memory_space=pltpu.HBM)] * 2,
        8,
        2000,
        (VMEM,) * 3,
        [pltpu.VMEM((1, row_count), jnp.int32), pltpu.SemaphoreType.DMA((2,))],
    )(
        pltpu.with_memory_space_constraint(labeled, pltpu.HBM),
        pltpu.with_memory_space_constraint(own, pltpu.HBM),
    )
    products = call(gram_kernel, slabs(rows), [SMEM] + [VMEM] * 4, 16, 500)(
        core, keep, own_t, own, other
    )
    sheet = exchanged(products, NEAR)
    partial = call(sum_kernel, slabs(rows // lax.axis_size(NEAR)), [VMEM], 8, 50)(sheet)
    partial, damping = lax.optimization_barrier((partial, damping))
    partials = [partial, *from_others(partial, FAR)]
    damping_other = lax.ppermute(damping, "layer", swap)
    damps = call(damp_kernel, slabs(16), [SMEM] * 2, 8, 50)(damping, damping_other)
    *partials, damps = lax.optimization_barrier((*partials, damps))
    total = call(total_kernel, slabs(rows), [VMEM] * planes, 8, 50)(*partials)
    mine = exchanged(total, NEAR)
    theirs = lax.ppermute(mine, "layer", swap)
    first, hard = call(
        functools.partial(first_kernel, count),
        (matrix, jax.ShapeDtypeStruct((1,), jnp.int32)),
        [VMEM] * 2,
        16,
        3000,
        (VMEM, SMEM),
        [square] * 4,
    )(damps, mine)
    solved, score = call(
        functools.partial(solve_kernel, count),
        (
            jax.ShapeDtypeStruct((row_count, width), F32),
            jax.ShapeDtypeStruct((1, row_count), F32),
        ),
        [SMEM] * 2 + [VMEM] * 6,
        32,
        6000,
        (pl.BlockSpec(memory_space=pl.ANY), VMEM),
        [square] * 9 + [pltpu.VMEM((row_count, width), F32)] * 2 + [pltpu.SemaphoreType.DMA],
    )(core, hard, damps, mine, theirs, first, own, other)
    return solved[None], score.reshape(row_count)


def solution(mesh):
    torus = Mesh(mesh.devices.reshape(mesh.shape["layer"], 4, 2, 4, 4), ("layer", *EX))
    in_specs = (P("layer", EX, None), P(EX), P("layer"))
    out_specs = (P("layer", EX, None), P(EX))
    return jax.shard_map(
        on_device, mesh=torus, in_specs=in_specs, out_specs=out_specs, check_vma=False
    )
```

```python
import functools

import jax
import jax.numpy as jnp
from jax import lax
from jax.experimental import pallas as pl
from jax.experimental.pallas import tpu as pltpu
from jax.sharding import Mesh
from jax.sharding import PartitionSpec as P

EX = ("z_hi", "z_lo", "y", "x")
FAR, NEAR = EX[0], EX[1:]
F32, BF16 = jnp.float32, jnp.bfloat16
LANES = 128
HALF = LANES // 2
DIAGONAL = HALF + HALF // 2
RESIDUAL = 0.002
STEPS = 60
TILES = 4
REFINEMENTS = 3


def slab_rows(blocks):
    return DIAGONAL + (blocks - 1) * LANES + HALF


def dot(a, b, dims=((1,), (0,)), precision=None):
    return lax.dot_general(a, b, (dims, ((), ())), preferred_element_type=F32, precision=precision)


def split(a):
    high = a.astype(BF16)
    return high, (a - high.astype(F32)).astype(BF16)


def dot_split(a, b, dims=((1,), (0,))):
    total = dot(a[0], b[0], dims)
    if len(b) > 1:
        total = total + dot(a[0], b[1], dims)
    if len(a) > 1:
        total = total + dot(a[1], b[0], dims)
    return total


def dot_full(out_ref, a_ref, b, base_ref=None, dims=((1,), (0,))):
    tile = a_ref.shape[0] // TILES

    def step(t, _):
        at = pl.ds(pl.multiple_of(t * tile, tile), tile)
        product = dot(a_ref[at, :].astype(F32), b[...], dims, lax.Precision.HIGHEST)
        out_ref[at, :] = product if base_ref is None else base_ref[at, :].astype(F32) - product
        return 0

    lax.fori_loop(0, TILES, step, 0)


def mask_kernel(labeled_hbm, own_hbm, own_t_ref, own_ref, keep_ref, labeled_ref, sems):
    arriving = [
        pltpu.make_async_copy(own_hbm, own_ref, sems.at[0]),
        pltpu.make_async_copy(labeled_hbm, labeled_ref, sems.at[1]),
    ]
    for copy in arriving:
        copy.start()
    for copy in arriving:
        copy.wait()
    keep = (labeled_ref[...] > 0).astype(F32)
    own_t_ref[...] = (own_ref[...].astype(F32).T * keep).astype(BF16)
    keep_ref[...] = keep


def gram_kernel(core_ref, keep_ref, own_t_ref, own_ref, other_ref, out_ref):
    core = core_ref[0]
    keep = keep_ref[...]
    own_t, own, other = own_t_ref[...], own_ref[...], other_ref[...]
    blocks = own.shape[1] // LANES
    first_t = jnp.where(core == 0, own_t, (other.astype(F32).T * keep).astype(BF16))
    last = jnp.where(core == 0, other, own)
    both = jnp.concatenate([own, other], axis=1)
    slab = slab_rows(blocks)
    left = lax.broadcasted_iota(jnp.int32, (HALF // 2, LANES), 1) < HALF
    for i in range(blocks):
        rows = own_t[i * LANES : (i + 1) * LANES]
        product = dot(rows, both[:, i * LANES : (i + blocks) * LANES])
        start = i * slab
        out_ref[start : start + HALF] = product[:HALF, :LANES]
        upper, lower = product[HALF : HALF + HALF // 2, :LANES], product[HALF + HALF // 2 :, :LANES]
        start = i * slab + HALF
        out_ref[start : start + HALF // 2] = jnp.where(left, pltpu.roll(upper, HALF, 1), lower)
        for b in range(1, blocks):
            start = i * slab + DIAGONAL + (b - 1) * LANES
            out_ref[start : start + LANES] = product[:, b * LANES : (b + 1) * LANES]
        middle = dot(first_t[i * LANES : (i + 1) * LANES], last[:, i * LANES : (i + 1) * LANES])
        start = (i + 1) * slab - HALF
        out_ref[start : start + HALF] = jnp.where(core == 0, middle[:HALF], middle[HALF:])


def damp_kernel(damp_ref, damp_other_ref, damps_ref):
    damps_ref[:8] = jnp.full((8, LANES), damp_ref[0])
    damps_ref[8:] = jnp.full((8, LANES), damp_other_ref[0])


def sum_kernel(in_ref, out_ref):
    rows = out_ref.shape[0]
    total = in_ref[:rows]
    for part in range(1, in_ref.shape[0] // rows):
        total = total + in_ref[part * rows : (part + 1) * rows]
    out_ref[...] = total


def total_kernel(*refs):
    out_ref = refs[-1]
    total = refs[0][...]
    for ref in refs[1:-1]:
        total = total + ref[...]
    rows = total.shape[0]
    for copy in range(out_ref.shape[0] // rows):
        out_ref[copy * rows : (copy + 1) * rows] = total


def eye(width):
    rows = lax.broadcasted_iota(jnp.int32, (width, width), 0)
    return rows == lax.broadcasted_iota(jnp.int32, (width, width), 1)


def scales(s_ref):
    diagonal = jnp.where(eye(s_ref.shape[0]), s_ref[...], 0.0)
    row = lax.rsqrt(jnp.sum(diagonal, axis=0, keepdims=True))
    return lax.rsqrt(jnp.sum(diagonal, axis=1, keepdims=True)), row


def near_inverse(s_ref, x_ref):
    column, row = scales(s_ref)
    a = s_ref[...] * column * row
    one = eye(s_ref.shape[0]).astype(F32)
    e = one - a
    e1 = e.astype(BF16)
    e2 = dot(e1, e1).astype(BF16)
    x = one + e
    x = (x + dot(x.astype(BF16), e2)).astype(BF16)
    r = one - dot_split(split(a), (x,))
    r1 = r.astype(BF16)
    r2 = dot(r1, r1)
    x_ref[...] = (x.astype(F32) + dot(x, (r + r2).astype(BF16))) * column * row
    return jnp.logical_not(jnp.sum(r2 * r2) <= RESIDUAL**2)


def full_inverse(s_ref, x_ref, a_ref, r_ref, t_ref):
    width = s_ref.shape[0]

    def residual():
        dot_full(r_ref, a_ref, x_ref)
        r_ref[...] = eye(width).astype(F32) - r_ref[...]
        return jnp.sum(r_ref[...] * r_ref[...])

    column, row = scales(s_ref)
    a_ref[...] = s_ref[...] * column * row
    x_ref[...] = x_ref[...] / (column * row)
    norm = residual()
    contracts = norm < 0.25

    @pl.when(jnp.logical_not(contracts))
    def _():
        largest = jnp.max(jnp.sum(jnp.abs(a_ref[...]), axis=1, keepdims=True))
        x_ref[...] = jnp.where(eye(width), 1.0 / largest, 0.0)
        residual()

    def far(state):
        return jnp.logical_and(state[0] < STEPS, jnp.logical_not(state[1] <= RESIDUAL**2))

    def newton(state):
        dot_full(t_ref, x_ref, r_ref)
        x_ref[...] += t_ref[...]
        return state[0] + 1, residual()

    start = jnp.where(contracts, norm, jnp.float32(width))
    lax.while_loop(far, newton, (jnp.int32(0), start))
    dot_full(t_ref, x_ref, r_ref)
    column, row = scales(s_ref)
    x_ref[...] = (x_ref[...] + t_ref[...]) * column * row


def part(ref, i, start, rows, blocks, count):
    at = i * slab_rows(blocks) + start
    return ref[at : at + rows] * (1.0 / count)


def whole_part(ref, i, b, blocks, count):
    return part(ref, i, DIAGONAL + (b - 1) * LANES, LANES, blocks, count)


def diagonal_part(ref, i, blocks, count):
    upper = part(ref, i, 0, HALF, blocks, count)
    packed = part(ref, i, HALF, HALF // 2, blocks, count)
    corner = jnp.concatenate([pltpu.roll(packed, HALF, 1), packed], axis=0)
    left = lax.broadcasted_iota(jnp.int32, (HALF, LANES), 1) < HALF
    turned = jnp.concatenate([upper, corner], axis=0).T
    return jnp.concatenate([upper, jnp.where(left, turned[HALF:], corner)], axis=0)


def put(ref, i, j, block):
    ref[i * LANES : (i + 1) * LANES, j * LANES : (j + 1) * LANES] = block


def put_diagonal(ref, slabs_ref, damp, count):
    blocks = ref.shape[0] // LANES
    unit = eye(LANES)
    for i in range(blocks):
        put(ref, i, i, diagonal_part(slabs_ref, i, blocks, count) + jnp.where(unit, damp, 0.0))
        for j in range(i + 1, blocks):
            block = whole_part(slabs_ref, i, j - i, blocks, count)
            put(ref, i, j, block)
            put(ref, j, i, block.T)


def first_kernel(count, damp_ref, mine_ref, x_ref, hard_ref, s_ref, a_ref, r_ref, t_ref):
    put_diagonal(s_ref, mine_ref, damp_ref[:1], count)
    hard = near_inverse(s_ref, x_ref)
    hard_ref[0] = hard.astype(jnp.int32)

    @pl.when(hard)
    def _():
        full_inverse(s_ref, x_ref, a_ref, r_ref, t_ref)


def solve_kernel(
    count, core_ref, hard_ref, damps_ref, mine_ref, theirs_ref, first_ref, own_ref, other_ref,
    solved_ref, score_ref, s_ref, d_ref, c_ref, ct_ref, a_ref, x_ref, r_ref, t_ref, y_ref,
    left_ref, z_ref, sem,
):
    near = core_ref[0] == 0
    width = own_ref.shape[1]
    blocks = width // LANES
    damp, damp_other = damps_ref[:1], damps_ref[8:9]

    for i in range(blocks):
        for j in range(i):
            block = whole_part(mine_ref, i, j + blocks - i, blocks, count)
            put(c_ref, i, j, block)
            put(ct_ref, j, i, block.T)
            block = whole_part(theirs_ref, i, j + blocks - i, blocks, count)
            put(ct_ref, i, j, block)
            put(c_ref, j, i, block.T)
        last = slab_rows(blocks) - HALF
        mine = part(mine_ref, i, last, HALF, blocks, count)
        theirs = part(theirs_ref, i, last, HALF, blocks, count)
        block = jnp.concatenate([jnp.where(near, mine, theirs), jnp.where(near, theirs, mine)], 0)
        turned = block.T
        put(c_ref, i, i, jnp.where(near, block, turned))
        put(ct_ref, i, i, jnp.where(near, turned, block))
    put_diagonal(d_ref, theirs_ref, damp_other, count)

    first = split(first_ref[...])
    y_ref[...] = dot_split(first, split(c_ref[...]))
    s_ref[...] = d_ref[...] - dot_split(split(ct_ref[...]), split(y_ref[...]))

    hard = jnp.logical_or(near_inverse(s_ref, x_ref), hard_ref[0] > 0)
    leaving = pltpu.make_async_copy(z_ref, solved_ref, sem)

    def candidate_sum(terms):
        folded = terms[:, :LANES]
        for b in range(1, blocks):
            folded = folded + terms[:, b * LANES : (b + 1) * LANES]
        return jnp.sum(folded.T, axis=0, keepdims=True)

    def outputs(z_own, z_other):
        z_ref[...] = z_own
        leaving.start()
        gain = candidate_sum(own_ref[...].astype(F32) * z_own + other_ref[...].astype(F32) * z_other)
        wide = (z_own.shape[0] // LANES,)
        penalty = jnp.tile(damp, wide) * candidate_sum(z_own * z_own)
        penalty = penalty + jnp.tile(damp_other, wide) * candidate_sum(z_other * z_other)
        score_ref[...] = (gain - penalty) / (1.0 + gain)
        leaving.wait()

    own, y = (own_ref[...],), split(y_ref[...])
    left = other_ref[...].astype(F32) - dot_split(own, y)
    z_other = dot_split(split(left), split(x_ref[...]))
    z_own = dot_split(own, split(first_ref[...])) - dot_split(split(z_other), y, ((1,), (1,)))
    outputs(z_own, z_other)

    @pl.when(hard)
    def _():
        dot_full(y_ref, first_ref, c_ref)
        dot_full(s_ref, ct_ref, y_ref, d_ref)
        full_inverse(s_ref, x_ref, a_ref, r_ref, t_ref)
        count_rows = left_ref.shape[0]
        top, bottom = pl.ds(0, count_rows), pl.ds(count_rows, count_rows)
        z_own, z_other = a_ref.at[top], a_ref.at[bottom]
        rest_own, rest_other = r_ref.at[top], r_ref.at[bottom]
        step_own, step_other = t_ref.at[top], t_ref.at[bottom]
        put_diagonal(s_ref, mine_ref, damp, count)
        a_ref[...] = jnp.zeros_like(a_ref)
        rest_own[...] = own_ref[...].astype(F32)
        rest_other[...] = other_ref[...].astype(F32)

        def refine(_, carry):
            dot_full(left_ref, rest_own, y_ref, rest_other)
            dot_full(step_other, left_ref, x_ref)
            dot_full(left_ref, rest_own, first_ref)
            dot_full(step_own, step_other, y_ref, left_ref, ((1,), (1,)))
            a_ref[...] += t_ref[...]
            dot_full(left_ref, z_own, s_ref, own_ref)
            dot_full(rest_own, z_other, ct_ref, left_ref)
            dot_full(left_ref, z_own, c_ref, other_ref)
            dot_full(rest_other, z_other, d_ref, left_ref)
            return carry

        lax.fori_loop(0, REFINEMENTS, refine, 0)
        outputs(z_own[...], z_other[...])


SMEM = pl.BlockSpec(memory_space=pltpu.SMEM)
VMEM = pl.BlockSpec(memory_space=pltpu.VMEM)


def call(kernel, out_shape, in_specs, mebibytes, megaflops=0, out_specs=VMEM, scratch=()):
    return pl.pallas_call(
        kernel,
        out_shape=out_shape,
        in_specs=in_specs,
        out_specs=out_specs,
        scratch_shapes=scratch,
        compiler_params=pltpu.CompilerParams(vmem_limit_bytes=mebibytes * 2**20),
        cost_estimate=pl.CostEstimate(
            flops=megaflops * 10**6, bytes_accessed=2**20, transcendentals=0
        ),
    )


def exchanged(array, axis):
    devices = lax.axis_size(axis)
    parts = lax.all_to_all(array.reshape(devices, 1, -1), axis, 0, 0, tiled=True)
    return parts.reshape(array.shape)


def from_others(array, axis):
    devices = lax.axis_size(axis)
    shifts = sorted(range(1, devices), key=lambda shift: min(shift, devices - shift))
    return [
        lax.ppermute(array, axis, [(i, (i + shift) % devices) for i in range(devices)])
        for shift in shifts
    ]


def on_device(grads, labeled, damping):
    _, row_count, width = grads.shape
    count = row_count * lax.axis_size(EX)
    core = lax.axis_index("layer").astype(jnp.int32).reshape(1)
    swap = [(0, 1), (1, 0)]
    own = grads[0]
    labeled = labeled.reshape(1, row_count)
    other = lax.ppermute(own, "layer", swap)
    blocks = width // LANES
    rows = blocks * slab_rows(blocks)
    planes = lax.axis_size(FAR)
    square = pltpu.VMEM((width, width), F32)
    matrix = jax.ShapeDtypeStruct((width, width), F32)

    def slabs(length):
        return jax.ShapeDtypeStruct((length, LANES), F32)

    own_t, own, keep = call(
        mask_kernel,
        (
            jax.ShapeDtypeStruct((width, row_count), BF16),
            jax.ShapeDtypeStruct((row_count, width), BF16),
            jax.ShapeDtypeStruct((1, row_count), F32),
        ),
        [pl.BlockSpec(memory_space=pltpu.HBM)] * 2,
        8,
        2000,
        (VMEM,) * 3,
        [pltpu.VMEM((1, row_count), jnp.int32), pltpu.SemaphoreType.DMA((2,))],
    )(
        pltpu.with_memory_space_constraint(labeled, pltpu.HBM),
        pltpu.with_memory_space_constraint(own, pltpu.HBM),
    )
    damping_other = lax.ppermute(damping, "layer", swap)
    other, damping_other = lax.optimization_barrier((other, damping_other))
    products = call(gram_kernel, slabs(rows), [SMEM] + [VMEM] * 4, 16, 500)(
        core, keep, own_t, own, other
    )
    sheet = exchanged(products, NEAR)
    partial = call(sum_kernel, slabs(rows // lax.axis_size(NEAR)), [VMEM], 8, 50)(sheet)
    partial, damping_other = lax.optimization_barrier((partial, damping_other))
    partials = [partial, *from_others(partial, FAR)]
    damps = call(damp_kernel, slabs(16), [SMEM] * 2, 8, 50)(damping, damping_other)
    *partials, damps = lax.optimization_barrier((*partials, damps))
    total = call(total_kernel, slabs(rows), [VMEM] * planes, 8, 50)(*partials)
    mine = exchanged(total, NEAR)
    theirs = lax.ppermute(mine, "layer", swap)
    first, hard = call(
        functools.partial(first_kernel, count),
        (matrix, jax.ShapeDtypeStruct((1,), jnp.int32)),
        [VMEM] * 2,
        16,
        3000,
        (VMEM, SMEM),
        [square] * 4,
    )(damps, mine)
    solved, score = call(
        functools.partial(solve_kernel, count),
        (
            jax.ShapeDtypeStruct((row_count, width), F32),
            jax.ShapeDtypeStruct((1, row_count), F32),
        ),
        [SMEM] * 2 + [VMEM] * 6,
        32,
        6000,
        (pl.BlockSpec(memory_space=pl.ANY), VMEM),
        [square] * 9 + [pltpu.VMEM((row_count, width), F32)] * 2 + [pltpu.SemaphoreType.DMA],
    )(core, hard, damps, mine, theirs, first, own, other)
    return solved[None], score.reshape(row_count)


def solution(mesh):
    torus = Mesh(mesh.devices.reshape(mesh.shape["layer"], 4, 2, 4, 4), ("layer", *EX))
    in_specs = (P("layer", EX, None), P(EX), P("layer"))
    out_specs = (P("layer", EX, None), P(EX))
    return jax.shard_map(
        on_device, mesh=torus, in_specs=in_specs, out_specs=out_specs, check_vma=False
    )
```

```python
import functools

import jax
import jax.numpy as jnp
from jax import lax
from jax.experimental import pallas as pl
from jax.experimental.pallas import tpu as pltpu
from jax.sharding import Mesh
from jax.sharding import PartitionSpec as P

EX = ("z_hi", "z_lo", "y", "x")
FAR, NEAR = EX[0], EX[1:]
F32, BF16 = jnp.float32, jnp.bfloat16
LANES = 128
HALF = LANES // 2
DIAGONAL = HALF + HALF // 2
RESIDUAL = 0.002
STEPS = 60
TILES = 4
REFINEMENTS = 3


def slab_rows(blocks):
    return DIAGONAL + (blocks - 1) * LANES + HALF


def dot(a, b, dims=((1,), (0,)), precision=None):
    return lax.dot_general(a, b, (dims, ((), ())), preferred_element_type=F32, precision=precision)


def split(a):
    high = a.astype(BF16)
    return high, (a - high.astype(F32)).astype(BF16)


def dot_split(a, b, dims=((1,), (0,))):
    total = dot(a[0], b[0], dims)
    if len(b) > 1:
        total = total + dot(a[0], b[1], dims)
    if len(a) > 1:
        total = total + dot(a[1], b[0], dims)
    return total


def dot_full(out_ref, a_ref, b, base_ref=None, dims=((1,), (0,))):
    tile = a_ref.shape[0] // TILES

    def step(t, _):
        at = pl.ds(pl.multiple_of(t * tile, tile), tile)
        product = dot(a_ref[at, :].astype(F32), b[...], dims, lax.Precision.HIGHEST)
        out_ref[at, :] = product if base_ref is None else base_ref[at, :].astype(F32) - product
        return 0

    lax.fori_loop(0, TILES, step, 0)


def mask_kernel(labeled_hbm, own_hbm, own_t_ref, own_ref, keep_ref, labeled_ref, sems):
    arriving = [
        pltpu.make_async_copy(own_hbm, own_ref, sems.at[0]),
        pltpu.make_async_copy(labeled_hbm, labeled_ref, sems.at[1]),
    ]
    for copy in arriving:
        copy.start()
    for copy in arriving:
        copy.wait()
    keep = (labeled_ref[...] > 0).astype(F32)
    own_t_ref[...] = (own_ref[...].astype(F32).T * keep).astype(BF16)
    keep_ref[...] = keep


def gram_kernel(core_ref, damp_ref, keep_ref, own_t_ref, own_ref, other_ref, out_ref):
    share = jnp.where(eye(LANES), damp_ref[0] * own_ref.shape[0], 0.0)
    core = core_ref[0]
    keep = keep_ref[...]
    own_t, own, other = own_t_ref[...], own_ref[...], other_ref[...]
    blocks = own.shape[1] // LANES
    first_t = jnp.where(core == 0, own_t, (other.astype(F32).T * keep).astype(BF16))
    last = jnp.where(core == 0, other, own)
    both = jnp.concatenate([own, other], axis=1)
    slab = slab_rows(blocks)
    left = lax.broadcasted_iota(jnp.int32, (HALF // 2, LANES), 1) < HALF
    for i in range(blocks):
        rows = own_t[i * LANES : (i + 1) * LANES]
        product = dot(rows, both[:, i * LANES : (i + blocks) * LANES])
        start = i * slab
        diagonal = product[:, :LANES] + share
        out_ref[start : start + HALF] = diagonal[:HALF]
        upper, lower = diagonal[HALF:DIAGONAL], diagonal[DIAGONAL:]
        start = i * slab + HALF
        out_ref[start : start + HALF // 2] = jnp.where(left, pltpu.roll(upper, HALF, 1), lower)
        for b in range(1, blocks):
            start = i * slab + DIAGONAL + (b - 1) * LANES
            out_ref[start : start + LANES] = product[:, b * LANES : (b + 1) * LANES]
        middle = dot(first_t[i * LANES : (i + 1) * LANES], last[:, i * LANES : (i + 1) * LANES])
        start = (i + 1) * slab - HALF
        out_ref[start : start + HALF] = jnp.where(core == 0, middle[:HALF], middle[HALF:])


def sum_kernel(in_ref, out_ref):
    rows = out_ref.shape[0]
    total = in_ref[:rows]
    for part in range(1, in_ref.shape[0] // rows):
        total = total + in_ref[part * rows : (part + 1) * rows]
    out_ref[...] = total


def total_kernel(*refs):
    out_ref = refs[-1]
    total = refs[0][...]
    for ref in refs[1:-1]:
        total = total + ref[...]
    rows = total.shape[0]
    for copy in range(out_ref.shape[0] // rows):
        out_ref[copy * rows : (copy + 1) * rows] = total


def eye(width):
    rows = lax.broadcasted_iota(jnp.int32, (width, width), 0)
    return rows == lax.broadcasted_iota(jnp.int32, (width, width), 1)


def scales(s_ref):
    diagonal = jnp.where(eye(s_ref.shape[0]), s_ref[...], 0.0)
    row = lax.rsqrt(jnp.sum(diagonal, axis=0, keepdims=True))
    return lax.rsqrt(jnp.sum(diagonal, axis=1, keepdims=True)), row


def near_inverse(s_ref, x_ref):
    column, row = scales(s_ref)
    a = s_ref[...] * column * row
    one = eye(s_ref.shape[0]).astype(F32)
    e = one - a
    e1 = e.astype(BF16)
    e2 = dot(e1, e1).astype(BF16)
    x = one + e
    x = (x + dot(x.astype(BF16), e2)).astype(BF16)
    r = one - dot_split(split(a), (x,))
    r1 = r.astype(BF16)
    r2 = dot(r1, r1)
    x_ref[...] = (x.astype(F32) + dot(x, (r + r2).astype(BF16))) * column * row
    return jnp.logical_not(jnp.sum(r2 * r2) <= RESIDUAL**2)


def full_inverse(s_ref, x_ref, a_ref, r_ref, t_ref):
    width = s_ref.shape[0]

    def residual():
        dot_full(r_ref, a_ref, x_ref)
        r_ref[...] = eye(width).astype(F32) - r_ref[...]
        return jnp.sum(r_ref[...] * r_ref[...])

    column, row = scales(s_ref)
    a_ref[...] = s_ref[...] * column * row
    x_ref[...] = x_ref[...] / (column * row)
    norm = residual()
    contracts = norm < 0.25

    @pl.when(jnp.logical_not(contracts))
    def _():
        largest = jnp.max(jnp.sum(jnp.abs(a_ref[...]), axis=1, keepdims=True))
        x_ref[...] = jnp.where(eye(width), 1.0 / largest, 0.0)
        residual()

    def far(state):
        return jnp.logical_and(state[0] < STEPS, jnp.logical_not(state[1] <= RESIDUAL**2))

    def newton(state):
        dot_full(t_ref, x_ref, r_ref)
        x_ref[...] += t_ref[...]
        return state[0] + 1, residual()

    start = jnp.where(contracts, norm, jnp.float32(width))
    lax.while_loop(far, newton, (jnp.int32(0), start))
    dot_full(t_ref, x_ref, r_ref)
    column, row = scales(s_ref)
    x_ref[...] = (x_ref[...] + t_ref[...]) * column * row


def part(ref, i, start, rows, blocks, count):
    at = i * slab_rows(blocks) + start
    return ref[at : at + rows] * (1.0 / count)


def whole_part(ref, i, b, blocks, count):
    return part(ref, i, DIAGONAL + (b - 1) * LANES, LANES, blocks, count)


def diagonal_part(ref, i, blocks, count):
    upper = part(ref, i, 0, HALF, blocks, count)
    packed = part(ref, i, HALF, HALF // 2, blocks, count)
    corner = jnp.concatenate([pltpu.roll(packed, HALF, 1), packed], axis=0)
    left = lax.broadcasted_iota(jnp.int32, (HALF, LANES), 1) < HALF
    turned = jnp.concatenate([upper, corner], axis=0).T
    return jnp.concatenate([upper, jnp.where(left, turned[HALF:], corner)], axis=0)


def put(ref, i, j, block):
    ref[i * LANES : (i + 1) * LANES, j * LANES : (j + 1) * LANES] = block


def put_diagonal(ref, slabs_ref, count):
    blocks = ref.shape[0] // LANES
    for i in range(blocks):
        put(ref, i, i, diagonal_part(slabs_ref, i, blocks, count))
        for j in range(i + 1, blocks):
            block = whole_part(slabs_ref, i, j - i, blocks, count)
            put(ref, i, j, block)
            put(ref, j, i, block.T)


def first_kernel(count, mine_ref, x_ref, hard_ref, s_ref, a_ref, r_ref, t_ref):
    put_diagonal(s_ref, mine_ref, count)
    hard = near_inverse(s_ref, x_ref)
    hard_ref[0] = hard.astype(jnp.int32)

    @pl.when(hard)
    def _():
        full_inverse(s_ref, x_ref, a_ref, r_ref, t_ref)


def solve_kernel(
    count, core_ref, hard_ref, damp_ref, damp_hbm, mine_ref, theirs_ref, first_ref, own_ref, other_ref,
    solved_ref, score_ref, s_ref, d_ref, c_ref, ct_ref, a_ref, x_ref, r_ref, t_ref, y_ref,
    left_ref, z_ref, damp_other_ref, sem, damp_sem,
):
    near = core_ref[0] == 0
    width = own_ref.shape[1]
    blocks = width // LANES
    damp_arriving = pltpu.make_async_copy(damp_hbm, damp_other_ref, damp_sem)
    damp_arriving.start()

    for i in range(blocks):
        for j in range(i):
            block = whole_part(mine_ref, i, j + blocks - i, blocks, count)
            put(c_ref, i, j, block)
            put(ct_ref, j, i, block.T)
            block = whole_part(theirs_ref, i, j + blocks - i, blocks, count)
            put(ct_ref, i, j, block)
            put(c_ref, j, i, block.T)
        last = slab_rows(blocks) - HALF
        mine = part(mine_ref, i, last, HALF, blocks, count)
        theirs = part(theirs_ref, i, last, HALF, blocks, count)
        block = jnp.concatenate([jnp.where(near, mine, theirs), jnp.where(near, theirs, mine)], 0)
        turned = block.T
        put(c_ref, i, i, jnp.where(near, block, turned))
        put(ct_ref, i, i, jnp.where(near, turned, block))
    put_diagonal(d_ref, theirs_ref, count)

    first = split(first_ref[...])
    y_ref[...] = dot_split(first, split(c_ref[...]))
    s_ref[...] = d_ref[...] - dot_split(split(ct_ref[...]), split(y_ref[...]))

    hard = jnp.logical_or(near_inverse(s_ref, x_ref), hard_ref[0] > 0)
    leaving = pltpu.make_async_copy(z_ref, solved_ref, sem)

    def candidate_sum(terms):
        folded = terms[:, :LANES]
        for b in range(1, blocks):
            folded = folded + terms[:, b * LANES : (b + 1) * LANES]
        return jnp.sum(folded.T, axis=0, keepdims=True)

    def outputs(z_own, z_other):
        z_ref[...] = z_own
        leaving.start()
        gain = candidate_sum(own_ref[...].astype(F32) * z_own + other_ref[...].astype(F32) * z_other)
        penalty = damp_ref[0] * candidate_sum(z_own * z_own)
        penalty = penalty + damp_other_ref[0] * candidate_sum(z_other * z_other)
        score_ref[...] = (gain - penalty) / (1.0 + gain)
        leaving.wait()

    own, y = (own_ref[...],), split(y_ref[...])
    left = other_ref[...].astype(F32) - dot_split(own, y)
    z_other = dot_split(split(left), split(x_ref[...]))
    z_own = dot_split(own, split(first_ref[...])) - dot_split(split(z_other), y, ((1,), (1,)))
    damp_arriving.wait()
    outputs(z_own, z_other)

    @pl.when(hard)
    def _():
        dot_full(y_ref, first_ref, c_ref)
        dot_full(s_ref, ct_ref, y_ref, d_ref)
        full_inverse(s_ref, x_ref, a_ref, r_ref, t_ref)
        count_rows = left_ref.shape[0]
        top, bottom = pl.ds(0, count_rows), pl.ds(count_rows, count_rows)
        z_own, z_other = a_ref.at[top], a_ref.at[bottom]
        rest_own, rest_other = r_ref.at[top], r_ref.at[bottom]
        step_own, step_other = t_ref.at[top], t_ref.at[bottom]
        put_diagonal(s_ref, mine_ref, count)
        a_ref[...] = jnp.zeros_like(a_ref)
        rest_own[...] = own_ref[...].astype(F32)
        rest_other[...] = other_ref[...].astype(F32)

        def refine(_, carry):
            dot_full(left_ref, rest_own, y_ref, rest_other)
            dot_full(step_other, left_ref, x_ref)
            dot_full(left_ref, rest_own, first_ref)
            dot_full(step_own, step_other, y_ref, left_ref, ((1,), (1,)))
            a_ref[...] += t_ref[...]
            dot_full(left_ref, z_own, s_ref, own_ref)
            dot_full(rest_own, z_other, ct_ref, left_ref)
            dot_full(left_ref, z_own, c_ref, other_ref)
            dot_full(rest_other, z_other, d_ref, left_ref)
            return carry

        lax.fori_loop(0, REFINEMENTS, refine, 0)
        outputs(z_own[...], z_other[...])


SMEM = pl.BlockSpec(memory_space=pltpu.SMEM)
VMEM = pl.BlockSpec(memory_space=pltpu.VMEM)


def call(kernel, out_shape, in_specs, mebibytes, megaflops=0, out_specs=VMEM, scratch=()):
    return pl.pallas_call(
        kernel,
        out_shape=out_shape,
        in_specs=in_specs,
        out_specs=out_specs,
        scratch_shapes=scratch,
        compiler_params=pltpu.CompilerParams(vmem_limit_bytes=mebibytes * 2**20),
        cost_estimate=pl.CostEstimate(
            flops=megaflops * 10**6, bytes_accessed=2**20, transcendentals=0
        ),
    )


def exchanged(array, axis):
    devices = lax.axis_size(axis)
    parts = lax.all_to_all(array.reshape(devices, 1, -1), axis, 0, 0, tiled=True)
    return parts.reshape(array.shape)


def from_others(array, axis):
    devices = lax.axis_size(axis)
    shifts = sorted(range(1, devices), key=lambda shift: min(shift, devices - shift))
    return [
        lax.ppermute(array, axis, [(i, (i + shift) % devices) for i in range(devices)])
        for shift in shifts
    ]


def on_device(grads, labeled, damping):
    _, row_count, width = grads.shape
    count = row_count * lax.axis_size(EX)
    core = lax.axis_index("layer").astype(jnp.int32).reshape(1)
    swap = [(0, 1), (1, 0)]
    own = grads[0]
    labeled = labeled.reshape(1, row_count)
    other = lax.ppermute(own, "layer", swap)
    blocks = width // LANES
    rows = blocks * slab_rows(blocks)
    planes = lax.axis_size(FAR)
    square = pltpu.VMEM((width, width), F32)
    matrix = jax.ShapeDtypeStruct((width, width), F32)

    def slabs(length):
        return jax.ShapeDtypeStruct((length, LANES), F32)

    own_t, own, keep = call(
        mask_kernel,
        (
            jax.ShapeDtypeStruct((width, row_count), BF16),
            jax.ShapeDtypeStruct((row_count, width), BF16),
            jax.ShapeDtypeStruct((1, row_count), F32),
        ),
        [pl.BlockSpec(memory_space=pltpu.HBM)] * 2,
        8,
        2000,
        (VMEM,) * 3,
        [pltpu.VMEM((1, row_count), jnp.int32), pltpu.SemaphoreType.DMA((2,))],
    )(
        pltpu.with_memory_space_constraint(labeled, pltpu.HBM),
        pltpu.with_memory_space_constraint(own, pltpu.HBM),
    )
    damping_other = lax.ppermute(damping, "layer", swap)
    other, damping_other = lax.optimization_barrier((other, damping_other))
    products = call(gram_kernel, slabs(rows), [SMEM] * 2 + [VMEM] * 4, 16, 500)(
        core, damping, keep, own_t, own, other
    )
    sheet = exchanged(products, NEAR)
    partial = call(sum_kernel, slabs(rows // lax.axis_size(NEAR)), [VMEM], 8, 50)(sheet)
    partials = [partial, *from_others(partial, FAR)]
    total = call(total_kernel, slabs(rows), [VMEM] * planes, 8, 50)(*partials)
    mine = exchanged(total, NEAR)
    theirs = lax.ppermute(mine, "layer", swap)
    first, hard = call(
        functools.partial(first_kernel, count),
        (matrix, jax.ShapeDtypeStruct((1,), jnp.int32)),
        [VMEM],
        16,
        3000,
        (VMEM, SMEM),
        [square] * 4,
    )(mine)
    solved, score = call(
        functools.partial(solve_kernel, count),
        (
            jax.ShapeDtypeStruct((row_count, width), F32),
            jax.ShapeDtypeStruct((1, row_count), F32),
        ),
        [SMEM] * 3 + [pl.BlockSpec(memory_space=pltpu.HBM)] + [VMEM] * 5,
        32,
        6000,
        (pl.BlockSpec(memory_space=pl.ANY), VMEM),
        [square] * 9 + [pltpu.VMEM((row_count, width), F32)] * 2
        + [pltpu.SMEM((1,), F32), pltpu.SemaphoreType.DMA, pltpu.SemaphoreType.DMA],
    )(
        core,
        hard,
        damping,
        pltpu.with_memory_space_constraint(damping_other, pltpu.HBM),
        mine,
        theirs,
        first,
        own,
        other,
    )
    return solved[None], score.reshape(row_count)


def solution(mesh):
    torus = Mesh(mesh.devices.reshape(mesh.shape["layer"], 4, 2, 4, 4), ("layer", *EX))
    in_specs = (P("layer", EX, None), P(EX), P("layer"))
    out_specs = (P("layer", EX, None), P(EX))
    return jax.shard_map(
        on_device, mesh=torus, in_specs=in_specs, out_specs=out_specs, check_vma=False
    )
```

```python
import functools

import jax
import jax.numpy as jnp
from jax import lax
from jax.experimental import pallas as pl
from jax.experimental.pallas import tpu as pltpu
from jax.sharding import Mesh
from jax.sharding import PartitionSpec as P

EX = ("z_hi", "z_lo", "y", "x")
FAR, NEAR = EX[0], EX[1:]
F32, BF16 = jnp.float32, jnp.bfloat16
LANES = 128
HALF = LANES // 2
DIAGONAL = HALF + HALF // 2
RESIDUAL = 0.002
STEPS = 60
TILES = 4
REFINEMENTS = 3


def slab_rows(blocks):
    return DIAGONAL + (blocks - 1) * LANES + HALF


def dot(a, b, dims=((1,), (0,)), precision=None):
    return lax.dot_general(a, b, (dims, ((), ())), preferred_element_type=F32, precision=precision)


def split(a):
    high = a.astype(BF16)
    return high, (a - high.astype(F32)).astype(BF16)


def dot_split(a, b, dims=((1,), (0,))):
    total = dot(a[0], b[0], dims)
    if len(b) > 1:
        total = total + dot(a[0], b[1], dims)
    if len(a) > 1:
        total = total + dot(a[1], b[0], dims)
    return total


def dot_full(out_ref, a_ref, b, base_ref=None, dims=((1,), (0,))):
    tile = a_ref.shape[0] // TILES

    def step(t, _):
        at = pl.ds(pl.multiple_of(t * tile, tile), tile)
        product = dot(a_ref[at, :].astype(F32), b[...], dims, lax.Precision.HIGHEST)
        out_ref[at, :] = product if base_ref is None else base_ref[at, :].astype(F32) - product
        return 0

    lax.fori_loop(0, TILES, step, 0)


def mask_kernel(labeled_hbm, own_hbm, own_t_ref, own_ref, keep_ref, labeled_ref, sems):
    arriving = [
        pltpu.make_async_copy(own_hbm, own_ref, sems.at[0]),
        pltpu.make_async_copy(labeled_hbm, labeled_ref, sems.at[1]),
    ]
    for copy in arriving:
        copy.start()
    for copy in arriving:
        copy.wait()
    keep = (labeled_ref[...] > 0).astype(F32)
    own_t_ref[...] = (own_ref[...].astype(F32).T * keep).astype(BF16)
    keep_ref[...] = keep


def gram_kernel(core_ref, damp_ref, keep_ref, own_t_ref, own_ref, other_ref, out_ref):
    share = jnp.where(eye(LANES), damp_ref[0] * own_ref.shape[0], 0.0)
    core = core_ref[0]
    keep = keep_ref[...]
    own_t, own, other = own_t_ref[...], own_ref[...], other_ref[...]
    blocks = own.shape[1] // LANES
    first_t = jnp.where(core == 0, own_t, (other.astype(F32).T * keep).astype(BF16))
    last = jnp.where(core == 0, other, own)
    both = jnp.concatenate([own, other], axis=1)
    slab = slab_rows(blocks)
    left = lax.broadcasted_iota(jnp.int32, (HALF // 2, LANES), 1) < HALF
    for i in range(blocks):
        rows = own_t[i * LANES : (i + 1) * LANES]
        product = dot(rows, both[:, i * LANES : (i + blocks) * LANES])
        start = i * slab
        diagonal = product[:, :LANES] + share
        out_ref[start : start + HALF] = diagonal[:HALF]
        upper, lower = diagonal[HALF:DIAGONAL], diagonal[DIAGONAL:]
        start = i * slab + HALF
        out_ref[start : start + HALF // 2] = jnp.where(left, pltpu.roll(upper, HALF, 1), lower)
        for b in range(1, blocks):
            start = i * slab + DIAGONAL + (b - 1) * LANES
            out_ref[start : start + LANES] = product[:, b * LANES : (b + 1) * LANES]
        middle = dot(first_t[i * LANES : (i + 1) * LANES], last[:, i * LANES : (i + 1) * LANES])
        start = (i + 1) * slab - HALF
        out_ref[start : start + HALF] = jnp.where(core == 0, middle[:HALF], middle[HALF:])


def sum_kernel(in_ref, out_ref):
    rows = out_ref.shape[0]
    total = in_ref[:rows]
    for part in range(1, in_ref.shape[0] // rows):
        total = total + in_ref[part * rows : (part + 1) * rows]
    out_ref[...] = total


def total_kernel(*refs):
    out_ref = refs[-1]
    total = refs[0][...]
    for ref in refs[1:-1]:
        total = total + ref[...]
    rows = total.shape[0]
    for copy in range(out_ref.shape[0] // rows):
        out_ref[copy * rows : (copy + 1) * rows] = total


def eye(width):
    rows = lax.broadcasted_iota(jnp.int32, (width, width), 0)
    return rows == lax.broadcasted_iota(jnp.int32, (width, width), 1)


def scales(s_ref):
    diagonal = jnp.where(eye(s_ref.shape[0]), s_ref[...], 0.0)
    row = lax.rsqrt(jnp.sum(diagonal, axis=0, keepdims=True))
    return lax.rsqrt(jnp.sum(diagonal, axis=1, keepdims=True)), row


def near_inverse(s_ref, x_ref):
    column, row = scales(s_ref)
    a = s_ref[...] * column * row
    one = eye(s_ref.shape[0]).astype(F32)
    e = one - a
    e1 = e.astype(BF16)
    e2 = dot(e1, e1).astype(BF16)
    x = one + e
    x = (x + dot(x.astype(BF16), e2)).astype(BF16)
    r = one - dot_split(split(a), (x,))
    r1 = r.astype(BF16)
    r2 = dot(r1, r1)
    x_ref[...] = (x.astype(F32) + dot(x, (r + r2).astype(BF16))) * column * row
    return jnp.logical_not(jnp.sum(r2 * r2) <= RESIDUAL**2)


def full_inverse(s_ref, x_ref, a_ref, r_ref, t_ref):
    width = s_ref.shape[0]

    def residual():
        dot_full(r_ref, a_ref, x_ref)
        r_ref[...] = eye(width).astype(F32) - r_ref[...]
        return jnp.sum(r_ref[...] * r_ref[...])

    column, row = scales(s_ref)
    a_ref[...] = s_ref[...] * column * row
    x_ref[...] = x_ref[...] / (column * row)
    norm = residual()
    contracts = norm < 0.25

    @pl.when(jnp.logical_not(contracts))
    def _():
        largest = jnp.max(jnp.sum(jnp.abs(a_ref[...]), axis=1, keepdims=True))
        x_ref[...] = jnp.where(eye(width), 1.0 / largest, 0.0)
        residual()

    def far(state):
        return jnp.logical_and(state[0] < STEPS, jnp.logical_not(state[1] <= RESIDUAL**2))

    def newton(state):
        dot_full(t_ref, x_ref, r_ref)
        x_ref[...] += t_ref[...]
        return state[0] + 1, residual()

    start = jnp.where(contracts, norm, jnp.float32(width))
    lax.while_loop(far, newton, (jnp.int32(0), start))
    dot_full(t_ref, x_ref, r_ref)
    column, row = scales(s_ref)
    x_ref[...] = (x_ref[...] + t_ref[...]) * column * row


def part(ref, i, start, rows, blocks, count):
    at = i * slab_rows(blocks) + start
    return ref[at : at + rows] * (1.0 / count)


def whole_part(ref, i, b, blocks, count):
    return part(ref, i, DIAGONAL + (b - 1) * LANES, LANES, blocks, count)


def diagonal_part(ref, i, blocks, count):
    upper = part(ref, i, 0, HALF, blocks, count)
    packed = part(ref, i, HALF, HALF // 2, blocks, count)
    corner = jnp.concatenate([pltpu.roll(packed, HALF, 1), packed], axis=0)
    left = lax.broadcasted_iota(jnp.int32, (HALF, LANES), 1) < HALF
    turned = jnp.concatenate([upper, corner], axis=0).T
    return jnp.concatenate([upper, jnp.where(left, turned[HALF:], corner)], axis=0)


def put(ref, i, j, block):
    ref[i * LANES : (i + 1) * LANES, j * LANES : (j + 1) * LANES] = block


def put_diagonal(ref, slabs_ref, count):
    blocks = ref.shape[0] // LANES
    for i in range(blocks):
        put(ref, i, i, diagonal_part(slabs_ref, i, blocks, count))
        for j in range(i + 1, blocks):
            block = whole_part(slabs_ref, i, j - i, blocks, count)
            put(ref, i, j, block)
            put(ref, j, i, block.T)


def first_kernel(
    count, damp_hbm, mine_ref, x_ref, hard_ref, damp_row_ref, s_ref, a_ref, r_ref, t_ref, damp_ref, sem
):
    arriving = pltpu.make_async_copy(damp_hbm, damp_ref, sem)
    arriving.start()
    put_diagonal(s_ref, mine_ref, count)
    hard = near_inverse(s_ref, x_ref)
    hard_ref[0] = hard.astype(jnp.int32)

    @pl.when(hard)
    def _():
        full_inverse(s_ref, x_ref, a_ref, r_ref, t_ref)

    arriving.wait()
    damp_row_ref[...] = jnp.full(damp_row_ref.shape, damp_ref[0])


def solve_kernel(
    count, core_ref, hard_ref, damp_ref, damp_row_ref, mine_ref, theirs_ref, first_ref, own_ref, other_ref,
    solved_ref, score_ref, s_ref, d_ref, c_ref, ct_ref, a_ref, x_ref, r_ref, t_ref, y_ref,
    left_ref, z_ref, sem,
):
    near = core_ref[0] == 0
    width = own_ref.shape[1]
    blocks = width // LANES
    damp_other = damp_row_ref[:1]

    for i in range(blocks):
        for j in range(i):
            block = whole_part(mine_ref, i, j + blocks - i, blocks, count)
            put(c_ref, i, j, block)
            put(ct_ref, j, i, block.T)
            block = whole_part(theirs_ref, i, j + blocks - i, blocks, count)
            put(ct_ref, i, j, block)
            put(c_ref, j, i, block.T)
        last = slab_rows(blocks) - HALF
        mine = part(mine_ref, i, last, HALF, blocks, count)
        theirs = part(theirs_ref, i, last, HALF, blocks, count)
        block = jnp.concatenate([jnp.where(near, mine, theirs), jnp.where(near, theirs, mine)], 0)
        turned = block.T
        put(c_ref, i, i, jnp.where(near, block, turned))
        put(ct_ref, i, i, jnp.where(near, turned, block))
    put_diagonal(d_ref, theirs_ref, count)

    first = split(first_ref[...])
    y_ref[...] = dot_split(first, split(c_ref[...]))
    s_ref[...] = d_ref[...] - dot_split(split(ct_ref[...]), split(y_ref[...]))

    hard = jnp.logical_or(near_inverse(s_ref, x_ref), hard_ref[0] > 0)
    leaving = pltpu.make_async_copy(z_ref, solved_ref, sem)

    def candidate_sum(terms):
        folded = terms[:, :LANES]
        for b in range(1, blocks):
            folded = folded + terms[:, b * LANES : (b + 1) * LANES]
        return jnp.sum(folded.T, axis=0, keepdims=True)

    def outputs(z_own, z_other):
        z_ref[...] = z_own
        leaving.start()
        gain = candidate_sum(own_ref[...].astype(F32) * z_own + other_ref[...].astype(F32) * z_other)
        penalty = damp_ref[0] * candidate_sum(z_own * z_own)
        wide = (z_own.shape[0] // LANES,)
        penalty = penalty + jnp.tile(damp_other, wide) * candidate_sum(z_other * z_other)
        score_ref[...] = (gain - penalty) / (1.0 + gain)
        leaving.wait()

    own, y = (own_ref[...],), split(y_ref[...])
    left = other_ref[...].astype(F32) - dot_split(own, y)
    z_other = dot_split(split(left), split(x_ref[...]))
    z_own = dot_split(own, split(first_ref[...])) - dot_split(split(z_other), y, ((1,), (1,)))
    outputs(z_own, z_other)

    @pl.when(hard)
    def _():
        dot_full(y_ref, first_ref, c_ref)
        dot_full(s_ref, ct_ref, y_ref, d_ref)
        full_inverse(s_ref, x_ref, a_ref, r_ref, t_ref)
        count_rows = left_ref.shape[0]
        top, bottom = pl.ds(0, count_rows), pl.ds(count_rows, count_rows)
        z_own, z_other = a_ref.at[top], a_ref.at[bottom]
        rest_own, rest_other = r_ref.at[top], r_ref.at[bottom]
        step_own, step_other = t_ref.at[top], t_ref.at[bottom]
        put_diagonal(s_ref, mine_ref, count)
        a_ref[...] = jnp.zeros_like(a_ref)
        rest_own[...] = own_ref[...].astype(F32)
        rest_other[...] = other_ref[...].astype(F32)

        def refine(_, carry):
            dot_full(left_ref, rest_own, y_ref, rest_other)
            dot_full(step_other, left_ref, x_ref)
            dot_full(left_ref, rest_own, first_ref)
            dot_full(step_own, step_other, y_ref, left_ref, ((1,), (1,)))
            a_ref[...] += t_ref[...]
            dot_full(left_ref, z_own, s_ref, own_ref)
            dot_full(rest_own, z_other, ct_ref, left_ref)
            dot_full(left_ref, z_own, c_ref, other_ref)
            dot_full(rest_other, z_other, d_ref, left_ref)
            return carry

        lax.fori_loop(0, REFINEMENTS, refine, 0)
        outputs(z_own[...], z_other[...])


SMEM = pl.BlockSpec(memory_space=pltpu.SMEM)
VMEM = pl.BlockSpec(memory_space=pltpu.VMEM)


def call(kernel, out_shape, in_specs, mebibytes, megaflops=0, out_specs=VMEM, scratch=()):
    return pl.pallas_call(
        kernel,
        out_shape=out_shape,
        in_specs=in_specs,
        out_specs=out_specs,
        scratch_shapes=scratch,
        compiler_params=pltpu.CompilerParams(vmem_limit_bytes=mebibytes * 2**20),
        cost_estimate=pl.CostEstimate(
            flops=megaflops * 10**6, bytes_accessed=2**20, transcendentals=0
        ),
    )


def exchanged(array, axis):
    devices = lax.axis_size(axis)
    parts = lax.all_to_all(array.reshape(devices, 1, -1), axis, 0, 0, tiled=True)
    return parts.reshape(array.shape)


def from_others(array, axis):
    devices = lax.axis_size(axis)
    shifts = sorted(range(1, devices), key=lambda shift: min(shift, devices - shift))
    return [
        lax.ppermute(array, axis, [(i, (i + shift) % devices) for i in range(devices)])
        for shift in shifts
    ]


def on_device(grads, labeled, damping):
    _, row_count, width = grads.shape
    count = row_count * lax.axis_size(EX)
    core = lax.axis_index("layer").astype(jnp.int32).reshape(1)
    swap = [(0, 1), (1, 0)]
    own = grads[0]
    labeled = labeled.reshape(1, row_count)
    other = lax.ppermute(own, "layer", swap)
    blocks = width // LANES
    rows = blocks * slab_rows(blocks)
    planes = lax.axis_size(FAR)
    square = pltpu.VMEM((width, width), F32)
    matrix = jax.ShapeDtypeStruct((width, width), F32)

    def slabs(length):
        return jax.ShapeDtypeStruct((length, LANES), F32)

    own_t, own, keep = call(
        mask_kernel,
        (
            jax.ShapeDtypeStruct((width, row_count), BF16),
            jax.ShapeDtypeStruct((row_count, width), BF16),
            jax.ShapeDtypeStruct((1, row_count), F32),
        ),
        [pl.BlockSpec(memory_space=pltpu.HBM)] * 2,
        8,
        2000,
        (VMEM,) * 3,
        [pltpu.VMEM((1, row_count), jnp.int32), pltpu.SemaphoreType.DMA((2,))],
    )(
        pltpu.with_memory_space_constraint(labeled, pltpu.HBM),
        pltpu.with_memory_space_constraint(own, pltpu.HBM),
    )
    damping_other = lax.ppermute(damping, "layer", swap)
    other, damping_other = lax.optimization_barrier((other, damping_other))
    products = call(gram_kernel, slabs(rows), [SMEM] * 2 + [VMEM] * 4, 16, 500)(
        core, damping, keep, own_t, own, other
    )
    sheet = exchanged(products, NEAR)
    partial = call(sum_kernel, slabs(rows // lax.axis_size(NEAR)), [VMEM], 8, 50)(sheet)
    partials = [partial, *from_others(partial, FAR)]
    total = call(total_kernel, slabs(rows), [VMEM] * planes, 8, 50)(*partials)
    mine = exchanged(total, NEAR)
    theirs = lax.ppermute(mine, "layer", swap)
    first, hard, damp_row = call(
        functools.partial(first_kernel, count),
        (matrix, jax.ShapeDtypeStruct((1,), jnp.int32), slabs(8)),
        [pl.BlockSpec(memory_space=pltpu.HBM), VMEM],
        16,
        3000,
        (VMEM, SMEM, VMEM),
        [square] * 4 + [pltpu.SMEM((1,), F32), pltpu.SemaphoreType.DMA],
    )(pltpu.with_memory_space_constraint(damping_other, pltpu.HBM), mine)
    solved, score = call(
        functools.partial(solve_kernel, count),
        (
            jax.ShapeDtypeStruct((row_count, width), F32),
            jax.ShapeDtypeStruct((1, row_count), F32),
        ),
        [SMEM] * 3 + [VMEM] * 6,
        32,
        6000,
        (pl.BlockSpec(memory_space=pl.ANY), VMEM),
        [square] * 9 + [pltpu.VMEM((row_count, width), F32)] * 2 + [pltpu.SemaphoreType.DMA],
    )(
        core,
        hard,
        damping,
        damp_row,
        mine,
        theirs,
        first,
        own,
        other,
    )
    return solved[None], score.reshape(row_count)


def solution(mesh):
    torus = Mesh(mesh.devices.reshape(mesh.shape["layer"], 4, 2, 4, 4), ("layer", *EX))
    in_specs = (P("layer", EX, None), P(EX), P("layer"))
    out_specs = (P("layer", EX, None), P(EX))
    return jax.shard_map(
        on_device, mesh=torus, in_specs=in_specs, out_specs=out_specs, check_vma=False
    )
```
